32 devices in a mesh: tm: 16 (over z, y, x), batch: 2 (over core).
Axes of the slice: x: 2, y: 2, z: 4, core: 2. Of those that a mesh axis runs over, the one named last changes fastest.
Arguments:
- state_map: float32 [512, 256, 256], P(('batch', 'tm')), parts along dimension 0, may hold values from -0.375 to 0.375
- input_map: float32 [512, 64, 256], P(('batch', 'tm')), parts along dimension 0, may hold values from -0.375 to 0.375
- closed_loop: float32 [512, 256, 256], P(('batch', 'tm')), parts along dimension 0, may hold values from -1.001 to 1.001
- feedback: float32 [512, 64, 256], P(('batch', 'tm')), parts along dimension 0, may hold values from -0.375 to 0.375
- value_matrix: float32 [512, 256, 256], P(('batch', 'tm')), parts along dimension 0, may hold values from -0.046875 to 1.5, as said below
- gain_inverse: float32 [512, 64, 64], P(('batch', 'tm')), parts along dimension 0, may hold values from -0.0105 to 0.2, as said below
- input_weight: float32 [128, 64], P('batch'), parts along dimension 0, may hold values from -0.36 to 6, as said below
- state_weight: float32 [512, 256], P(('batch', 'tm')), parts along dimension 0, may hold values from 0.1 to 3
- state_linear: float32 [512, 256], P(('batch', 'tm')), parts along dimension 0, may hold values from -0.18 to 0.18
- input_linear: float32 [512, 64], P(('batch', 'tm')), parts along dimension 0, may hold values from -0.18 to 0.18
- offset: float32 [512, 256], P(('batch', 'tm')), parts along dimension 0, may hold values from -0.18 to 0.18
- upper_bound: float32 [512, 64], P(('batch', 'tm')), parts along dimension 0, may hold values from 0.1 to 0.3
- states: float32 [512, 256], P(('batch', 'tm')), parts along dimension 0, may hold values from -0.18 to 0.18
- inputs: float32 [512, 64], P(('batch', 'tm')), parts along dimension 0, may hold values from -0.18 to 0.18
- multipliers: float32 [512, 256], P(('batch', 'tm')), parts along dimension 0, may hold values from -0.18 to 0.18
- bound_mult: float32 [512, 64], P(('batch', 'tm')), parts along dimension 0, may hold values from 0 to 0.06
- active: int32 [512, 64], P(('batch', 'tm')), parts along dimension 0, may hold values 0 or 1
Outputs:
- state_step: float32 [512, 256], P(('batch', 'tm')), parts along dimension 0
- input_step: float32 [512, 64], P(('batch', 'tm')), parts along dimension 0
- multiplier_step: float32 [512, 256], P(('batch', 'tm')), parts along dimension 0
- bound_step: float32 [512, 64], P(('batch', 'tm')), parts along dimension 0
- kkt_norms: float32 [6], P('batch'), parts along dimension 0
The draws below stay inside these ranges and needn't reach their ends.
There are 2 independent parts, one for each index of `batch`. The reference program is written for one: setup_inputs(seed, part) draws one part's arguments, and reference() takes and returns one part's arrays. A program takes and returns all parts, laid end to end along the dimension named above; each array names one. Nothing has to cross between parts.
Inputs may be any that keep to these rules, and one draw needn't show every extreme that they name: `value_matrix`: each section's matrix is symmetric. `gain_inverse`: each section's matrix is symmetric. `input_weight`: symmetric.
All inputs are finite; a program needn't handle non-finite values. No bound on the sum of `active` on one device may be relied on, other than what follows from the above.
Results may differ from the reference program's by a relative error of at most 0.0003.
Values sent between devices are 32-bit elements; how exact they have to be, the bound alone decides.
A program may use at most 128 MiB of HBM per device.

```python
import math
import jax
import jax.numpy as jnp
from jax import lax

NS = 256
NU = 64
HORIZON = 256


def symmetric_draw(key, sections, dimension, lowest, highest, spread):
    first_key, second_key = jax.random.split(key)
    diagonal = jax.random.uniform(first_key, (sections, dimension), jnp.float32, lowest, highest)
    noise_raw = jax.random.normal(second_key, (sections, dimension, dimension), jnp.float32) * spread
    mixed = jnp.clip((noise_raw + jnp.swapaxes(noise_raw, 1, 2)) / math.sqrt(2.0), -3.0 * spread, 3.0 * spread)
    identity = jnp.eye(dimension, dtype=jnp.float32)
    return mixed * (1.0 - identity) + diagonal[:, :, None] * identity


def draw_value_matrix(key, part):
    return symmetric_draw(jax.random.fold_in(key, 11), HORIZON, NS, 0.5, 1.5, 0.25 / math.sqrt(NS))


def draw_gain_inverse(key, part):
    return symmetric_draw(jax.random.fold_in(key, 12), HORIZON, NU, 0.08, 0.2, 0.028 / math.sqrt(NU))


def draw_input_weight(key, part):
    return symmetric_draw(jax.random.fold_in(key, 13), 1, NU, 2.0, 6.0, 0.96 / math.sqrt(NU))[0]


def draw_closed_loop(key, part):
    subkeys = jax.random.split(jax.random.fold_in(key, 7), 5)
    ranking = jax.random.permutation(subkeys[0], NS)
    slow_total = NS // 2
    slow_channel = ranking < slow_total
    same_class = (slow_channel[:, None] == slow_channel[None, :]).astype(jnp.float32)
    slow_rate = jax.random.uniform(subkeys[1], (HORIZON, NS), jnp.float32, 0.3, 2.0) / HORIZON
    memory = jnp.exp(jax.random.uniform(subkeys[2], (HORIZON, NS), jnp.float32, math.log(2.0), math.log(8.0)))
    decays = jnp.where(slow_channel[None, :], jnp.exp(-slow_rate), jnp.exp(-1.0 / memory))
    noise_raw = jax.random.normal(subkeys[3], (HORIZON, NS, NS), jnp.float32) * (0.5 / math.sqrt(NS))
    cross_raw = jax.random.normal(subkeys[4], (HORIZON, NS, NS), jnp.float32) * (0.25 / math.sqrt(NS * HORIZON))
    within_part = (noise_raw - jnp.swapaxes(noise_raw, 1, 2)) * same_class
    between_part = (cross_raw - jnp.swapaxes(cross_raw, 1, 2)) * (1.0 - same_class)
    skew_part = within_part + between_part
    identity = jnp.eye(NS, dtype=jnp.float32)
    rotation = jnp.linalg.solve(identity + skew_part, identity - skew_part)
    return decays[:, :, None] * rotation


def with_ends(array, stream_key, low, top_value):
    spot = [jax.random.randint(jax.random.fold_in(stream_key, axis), (), 0, length) for axis, length in enumerate(array.shape)]
    main_axis = array.shape.index(max(array.shape))
    next_to = spot[:main_axis] + [(spot[main_axis] + 1) % array.shape[main_axis]] + spot[main_axis + 1:]
    return array.at[tuple(spot)].set(low).at[tuple(next_to)].set(top_value)


def block_scale(key, dims, shards, low, high):
    level = 1.0
    for axis_at, blocks in shards:
        draws = jax.random.uniform(jax.random.fold_in(jax.random.fold_in(key, 6), axis_at), (blocks,), jnp.float32, low / len(shards), high / len(shards))
        level = level * jnp.repeat(jnp.exp(draws), dims[axis_at] // blocks).reshape((-1,) + (1,) * (len(dims) - 1 - axis_at))
    return level


def noise(own_key, shape, scale, limit, cuts=(), kind=jnp.bfloat16):
    drawn = jax.random.normal(own_key, shape, jnp.float32) * scale
    if len(cuts) > 0:
        drawn = block_scale(own_key, shape, cuts, -0.22, 0.18) * drawn
    return jnp.clip(drawn, min=-limit, max=limit).astype(kind)


def setup_inputs(seed: int = 0, part: int = 0) -> dict:
    key_list = jax.random.split(jax.random.key(seed), 18)
    part_splits = jax.random.split(jax.random.fold_in(key_list[17], part), 18)
    state_map = noise(part_splits[0], (HORIZON, NS, NS), NS ** -0.5, 0.375, ((0, 16),), jnp.float32)
    input_map = noise(part_splits[1], (HORIZON, NU, NS), NS ** -0.5, 0.375, ((0, 16),), jnp.float32)
    closed_loop = draw_closed_loop(jax.random.fold_in(jax.random.fold_in(key_list[17], part), 71), part)
    feedback = noise(part_splits[3], (HORIZON, NU, NS), NS ** -0.5, 0.375, ((0, 16),), jnp.float32)
    value_matrix = draw_value_matrix(jax.random.fold_in(jax.random.fold_in(key_list[17], part), 71), part)
    gain_inverse = draw_gain_inverse(jax.random.fold_in(jax.random.fold_in(key_list[17], part), 71), part)
    input_weight = draw_input_weight(jax.random.fold_in(jax.random.fold_in(key_list[17], part), 71), part)
    state_weight = jnp.clip(jnp.exp(math.log(3.0) - 3.4011974 * jax.random.uniform(part_splits[7], (HORIZON, NS), jnp.float32) ** block_scale(part_splits[7], (HORIZON, NS), ((0, 16),), -0.2, 0.2)), 0.1, 3.0)
    state_linear = noise(part_splits[8], (HORIZON, NS), 0.03, 0.18, ((0, 16),), jnp.float32)
    input_linear = noise(part_splits[9], (HORIZON, NU), 0.03, 0.18, ((0, 16),), jnp.float32)
    offset = noise(part_splits[10], (HORIZON, NS), 0.03, 0.18, ((0, 16),), jnp.float32)
    upper_bound = jnp.clip(0.1 + 0.20000001043081284 * jax.random.uniform(part_splits[11], (HORIZON, NU), jnp.float32) ** block_scale(part_splits[11], (HORIZON, NU), ((0, 16),), -0.2, 0.2), 0.1, 0.3)
    states = noise(part_splits[12], (HORIZON, NS), 0.03, 0.18, ((0, 16),), jnp.float32)
    inputs = noise(part_splits[13], (HORIZON, NU), 0.03, 0.18, ((0, 16),), jnp.float32)
    multipliers = noise(part_splits[14], (HORIZON, NS), 0.03, 0.18, ((0, 16),), jnp.float32)
    bound_mult = jnp.clip(0.06 * jax.random.uniform(part_splits[15], (HORIZON, NU), jnp.float32) ** block_scale(part_splits[15], (HORIZON, NU), ((0, 16),), -0.2, 0.2), 0.0, 0.06)
    active = with_ends((jax.random.randint(part_splits[16], (HORIZON, NU), 0, 3) < 1).astype(jnp.int32), jax.random.fold_in(part_splits[16], 1), 0, 1)
    return dict(state_map=state_map, input_map=input_map, closed_loop=closed_loop, feedback=feedback, value_matrix=value_matrix, gain_inverse=gain_inverse, input_weight=input_weight, state_weight=state_weight, state_linear=state_linear, input_linear=input_linear, offset=offset, upper_bound=upper_bound, states=states, inputs=inputs, multipliers=multipliers, bound_mult=bound_mult, active=active)


PRECISE = lax.Precision.HIGHEST
floor_share = 0.001

def apply_each(matrices, vectors):
    return jnp.einsum('kij,kj->ki', matrices, vectors, precision=PRECISE)

def apply_transposed(matrices, vectors):
    return jnp.einsum('kji,kj->ki', matrices, vectors, precision=PRECISE)

def backward_sweep(loop_mats, sources, incoming):

    def section(costate, section_item):
        matrix, source = section_item
        earlier = jnp.dot(costate, matrix, precision=PRECISE) + source
        return (earlier, (costate, earlier))
    final_state, (after, before) = lax.scan(section, incoming, (loop_mats, sources), reverse=True)
    return (after, before, final_state)

def forward_sweep(loop_mats, defects, pushes, entering):

    def section(carried, section_item):
        matrix, defect, pushed = section_item
        correction = carried - defect
        return (jnp.dot(matrix, correction, precision=PRECISE) + pushed, correction)
    final_state, steps = lax.scan(section, entering, (loop_mats, defects, pushes))
    return (steps, final_state)

def make_statistics(defect, grad_state, grad_input, slack_gap, offset, state_linear, input_linear, bound_mult):
    return jnp.stack([jnp.sum(defect * defect), jnp.sum(grad_state * grad_state) + jnp.sum(grad_input * grad_input), jnp.sum(slack_gap * slack_gap), jnp.sum(offset * offset), jnp.sum(state_linear * state_linear) + jnp.sum(input_linear * input_linear), jnp.sum(bound_mult * bound_mult)])

def make_norms(totals, horizon, state_count, input_count):
    primal = totals[0] / (totals[3] + floor_share * horizon * state_count)
    dual = totals[1] / (totals[4] + floor_share * horizon * (state_count + input_count))
    complement = totals[2] / (totals[5] + floor_share * horizon * input_count)
    return jnp.sqrt(jnp.stack([primal, dual, complement]))

def reference(state_map, input_map, closed_loop, feedback, value_matrix, gain_inverse, input_weight, state_weight, state_linear, input_linear, offset, upper_bound, states, inputs, multipliers, bound_mult, active):
    state_count = states.shape[1]
    input_count = inputs.shape[1]
    horizon = states.shape[0]
    predicted = apply_each(state_map, states) + apply_transposed(input_map, inputs)
    previous = jnp.concatenate([jnp.zeros((1, state_count), jnp.float32), predicted[:-1]], axis=0)
    defect = states - previous - offset
    following = jnp.concatenate([multipliers[1:], jnp.zeros((1, state_count), jnp.float32)], axis=0)
    grad_state = state_weight * states + state_linear + multipliers - apply_transposed(state_map, following)
    grad_input = jnp.einsum('ij,kj->ki', input_weight, inputs, precision=PRECISE) + input_linear - apply_each(input_map, following) + bound_mult
    slack_gap = bound_mult * (upper_bound - inputs)
    sources = apply_each(value_matrix, defect) + grad_state + apply_transposed(feedback, grad_input)
    after, before, unused = backward_sweep(closed_loop, sources, jnp.zeros((state_count,), jnp.float32))
    pulled = apply_each(input_map, after)
    forward_gain = -apply_each(gain_inverse, grad_input + pulled)
    pushes = apply_transposed(input_map, forward_gain)
    state_step, unused_final = forward_sweep(closed_loop, defect, pushes, jnp.zeros((state_count,), jnp.float32))
    chosen = active.astype(jnp.float32)
    input_step = (1.0 - chosen) * (apply_each(feedback, state_step) + forward_gain) + chosen * (upper_bound - inputs)
    multiplier_step = apply_each(value_matrix, state_step - defect) + before
    bound_step = chosen * (grad_input + jnp.einsum('ij,kj->ki', input_weight, input_step, precision=PRECISE) + pulled)
    totals = make_statistics(defect, grad_state, grad_input, slack_gap, offset, state_linear, input_linear, bound_mult)
    kkt_norms = make_norms(totals, horizon, state_count, input_count)
    return (state_step, input_step, multiplier_step, bound_step, kkt_norms)
```

```python
import functools
import jax
import jax.numpy as jnp
from jax import lax
from jax.experimental import pallas as pl
from jax.experimental.pallas import tpu as pltpu
from jax.sharding import PartitionSpec as P

F32 = jnp.float32
BF16 = jnp.bfloat16
PRECISE = lax.Precision.HIGHEST
MESH = pl.DeviceIdType.MESH
floor_share = 0.001
LANES = 128
VMEM_LIMIT = 48 * 1024 * 1024


def parts_of(x):
    high = x.astype(BF16)
    return high, (x - high.astype(F32)).astype(BF16)


def matmul(a, b):
    ah, al = parts_of(a)
    bh, bl = parts_of(b)
    dot = functools.partial(jnp.dot, preferred_element_type=F32)
    return dot(ah, bh) + (dot(ah, bl) + dot(al, bh))


def turned(x):
    rows, cols = x.shape
    up = -rows % LANES
    side = -cols % LANES
    if up:
        x = jnp.concatenate([x, jnp.zeros((up, cols), F32)], axis=0)
    if side:
        x = jnp.concatenate([x, jnp.zeros((rows + up, side), F32)], axis=1)
    return x.T[:cols, :rows]


def column(row):
    return jnp.broadcast_to(row, (LANES, row.shape[1])).T[:, :1]


def row_of(col):
    return jnp.broadcast_to(col, (col.shape[0], LANES)).T[:1]


def times(matrix, row):
    return jnp.sum(matrix * row, axis=1, keepdims=True)


def times_t(matrix, col):
    return jnp.sum(matrix * col, axis=0, keepdims=True)


def kernel(n, size, *refs):
    (a_hbm, b_hbm, m_hbm, k_hbm, v_hbm, gi_hbm, w_hbm, sw_hbm, sl_hbm, il_hbm, of_hbm, ub_hbm,
     st_hbm, in_hbm, mu_hbm, bm_hbm, ac_hbm,
     packed_out,
     a, b, m, fb, v, gi, w, sw, sl, il, of, ub, st, inp, mu, bm, ac,
     pre, suf, group, whole, sources, pushes, back_local, fwd_local, back,
     cols, fol_in, prd_in, prd_out, fol_out, vec_b, vec_f, ch_b_in, ch_f_in, ch_b_out, ch_f_out,
     load_sem, m_sem, nb_send, nb_recv, p_send, p_recv, b_send, b_recv, f_send, f_recv,
     ch_send, ch_recv) = refs
    me = lax.axis_index("tm")
    place = lax.rem(me, size)
    base = me - place
    at_group = lax.div(me, size)
    groups = n // size
    sections, ns = st.shape
    nu = inp.shape[1]
    half = sections // 2

    order = []
    for i in range(half):
        order += [i, sections - 1 - i]
    for k in order:
        pltpu.make_async_copy(m_hbm.at[k], m.at[k], m_sem.at[k]).start()
    small = [(w_hbm, w), (sw_hbm, sw), (sl_hbm, sl), (il_hbm, il), (of_hbm, of), (ub_hbm, ub),
             (st_hbm, st), (in_hbm, inp), (mu_hbm, mu), (bm_hbm, bm), (ac_hbm, ac)]
    large = [(a_hbm, a), (b_hbm, b), (v_hbm, v), (k_hbm, fb), (gi_hbm, gi)]
    loads = [
        pltpu.make_async_copy(src, dst, load_sem.at[i]) for i, (src, dst) in enumerate(small + large)
    ]
    for load in loads:
        load.start()

    barrier = pltpu.get_barrier_semaphore()
    first_of, last_of = place == 0, place == size - 1
    relations = [
        (jnp.logical_and(first_of, me > 0), me - 1),
        (jnp.logical_and(last_of, me < n - 1), me + 1),
        (at_group > 0, me - size),
        (at_group < groups - 1, me + size),
    ]
    mates = [base + lax.rem(place + j, size) for j in range(1, size)]
    for mate in mates:
        pl.semaphore_signal(barrier, inc=1, device_id={"tm": mate}, device_id_type=MESH)
    for holds, peer in relations:
        @pl.when(holds)
        def _():
            pl.semaphore_signal(barrier, inc=1, device_id={"tm": peer}, device_id_type=MESH)
    def remote(src, dst, send, recv, peer):
        return pltpu.make_async_remote_copy(
            src_ref=src, dst_ref=dst, send_sem=send, recv_sem=recv,
            device_id={"tm": peer}, device_id_type=MESH,
        )

    for load in loads[: len(small)]:
        load.wait()
    to_earlier = remote(fol_out, fol_in, nb_send.at[0], nb_recv.at[0], me - 1)
    to_later = remote(prd_out, prd_in, nb_send.at[1], nb_recv.at[1], me + 1)
    fol_out[...] = jnp.broadcast_to(mu[0:1], fol_out.shape)

    def wait_loop(k):
        pltpu.make_async_copy(m_hbm.at[k], m.at[k], m_sem.at[k]).wait()

    wait_loop(0)
    wait_loop(sections - 1)
    pre[0] = m[0]
    suf[sections - 1] = m[sections - 1]

    def grow(i, waits):
        j = sections - 1 - i
        if waits:
            wait_loop(i)
            wait_loop(j)
        pre[i] = matmul(m[i], pre[i - 1])
        suf[j] = matmul(suf[j + 1], m[j])

    @pl.loop(1, half)
    def _(i):
        grow(i, True)

    product = matmul(suf[half], pre[half - 1])
    suf[0] = product
    group[pl.ds(place, 1)] = product[None]
    peers = size - 1
    for holds, peer in relations:
        peers = peers + jnp.where(holds, 1, 0)
    pl.semaphore_wait(barrier, peers)

    @pl.when(me > 0)
    def _():
        to_earlier.start()

    along = place + 1 - 2 * lax.rem(place, 2)
    across = place + 2 - 4 * lax.div(place, 2)
    far = size - 1 - place
    top, bottom = pl.ds(0, ns // 2), pl.ds(ns // 2, ns // 2)

    def whole_block(slot, j, peer):
        return remote(group.at[slot], group.at[slot], p_send.at[j], p_recv.at[j], base + peer)

    def half_block(slot, rows, j, peer):
        ref = group.at[slot, rows]
        return remote(ref, ref, p_send.at[j], p_recv.at[j], base + peer)

    if size == 4:
        p_copies = [whole_block(place, 0, along), whole_block(place, 1, across)]
    else:
        p_copies = [
            whole_block(place, j, lax.rem(place + j + 1, size)) for j in range(size - 1)
        ]
    for copy in p_copies:
        copy.start()

    for load in loads[len(small):]:
        load.wait()
    lane = lax.broadcasted_iota(jnp.int32, (ns, LANES), 1)
    lane_u = lax.broadcasted_iota(jnp.int32, (nu, LANES), 1)

    inputs_t = turned(inp[...])
    acc = jnp.zeros((ns, LANES), F32)
    for k in range(sections):
        acc = jnp.where(lane == k, times(a[k], st[k:k + 1]), acc)
    predicted = acc.T[:sections]
    rows = [times_t(b[k], inputs_t[:, k:k + 1]) for k in range(sections)]
    predicted = predicted + jnp.concatenate(rows, axis=0)
    prd_out[...] = jnp.broadcast_to(predicted[sections - 1:], prd_out.shape)

    @pl.when(me < n - 1)
    def _():
        to_later.start()

    @pl.loop(half, sections - 1)
    def _(i):
        grow(i, False)

    @pl.when(me < n - 1)
    def _():
        to_earlier.wait_recv()

    @pl.when(me == n - 1)
    def _():
        fol_in[...] = jnp.zeros_like(fol_in)

    following = jnp.concatenate([mu[1:], fol_in[0:1]], axis=0)
    following_t = turned(following)
    grad_input = (
        jnp.dot(inp[...], w[...], precision=PRECISE, preferred_element_type=F32) + il[...] + bm[...]
    )
    acc = jnp.zeros((nu, LANES), F32)
    for k in range(sections):
        acc = jnp.where(lane_u == k, times(b[k], following[k:k + 1]), acc)
    grad_input = grad_input - turned(acc)[:sections]
    grad_input_t = turned(grad_input)
    rows = [times_t(a[k], following_t[:, k:k + 1]) for k in range(sections)]
    grad_state = sw[...] * st[...] + sl[...] + mu[...] - jnp.concatenate(rows, axis=0)

    @pl.when(me > 0)
    def _():
        to_later.wait_recv()

    @pl.when(me == 0)
    def _():
        prd_in[...] = jnp.zeros_like(prd_in)

    previous = jnp.concatenate([prd_in[0:1], predicted[:sections - 1]], axis=0)
    defect = st[...] - previous - of[...]
    defect_t = turned(defect)
    rows = [
        times_t(v[k], defect_t[:, k:k + 1]) + times_t(fb[k], grad_input_t[:, k:k + 1])
        for k in range(sections)
    ]
    sources[...] = jnp.concatenate(rows, axis=0) + grad_state
    slack = bm[...] * (ub[...] - inp[...])

    def total(*xs):
        return sum(
            jnp.sum(jnp.sum(x * x, axis=1, keepdims=True), axis=0, keepdims=True) for x in xs
        )

    sums = [total(defect), total(grad_state, grad_input), total(slack), total(of[...]),
            total(sl[...], il[...]), total(bm[...])]
    line = lax.broadcasted_iota(jnp.int32, (1, ns), 1)
    stats = jnp.zeros((1, ns), F32)
    for i, value in enumerate(sums):
        stats = jnp.where(line == i, value, stats)

    def packed(vector, extra):
        return jnp.concatenate([vector, extra, jnp.zeros((6, ns), F32)], axis=0)

    sources_t = turned(sources[...])
    costate = sources[0:1]
    for k in range(1, sections):
        costate = costate + times_t(pre[k - 1], sources_t[:, k:k + 1])
    vec_b[pl.ds(place, 1)] = packed(costate, stats)[None]
    b_copies = [
        remote(vec_b.at[place], vec_b.at[place], b_send.at[j], b_recv.at[j], mate)
        for j, mate in enumerate(mates)
    ]
    for copy in b_copies:
        copy.start()

    def arrive(buffer, send, recv):
        for j in range(size - 1):
            source = base + lax.rem(place + size - 1 - j, size)
            slot = source - base
            remote(buffer.at[slot], buffer.at[slot], send.at[j], recv.at[j], source).wait_recv()

    if size == 4:
        whole_block(along, 0, along).wait_recv()
        second = half_block(along, top, 2, across)
        second.start()
        whole_block(across, 1, across).wait_recv()
        third = half_block(across, bottom, 3, along)
        third.start()
        p_copies = p_copies + [second, third]

    costate = sources[sections - 1:]
    back_local[sections - 1:] = costate
    for k in range(sections - 2, -1, -1):
        costate = times_t(m[k], column(costate)) + sources[k:k + 1]
        back_local[k:k + 1] = costate

    arrive(vec_b, b_send, b_recv)
    if size == 4:
        half_block(far, top, 2, across).wait_recv()
        half_block(far, bottom, 3, along).wait_recv()
    else:
        arrive(group, p_send, p_recv)
    joined = group[0]
    for e in range(1, size):
        joined = matmul(group[e], joined)
    whole[...] = joined
    group_stats = jnp.sum(vec_b[:, 1, :], axis=0, keepdims=True)

    y = vec_b[size - 1, 0:1]
    for e in range(size - 2, -1, -1):
        y = vec_b[e, 0:1] + times_t(group[e], column(y))
    to_before = remote(ch_b_out, ch_b_in, ch_send.at[0], ch_recv.at[0], me - size)
    to_after = remote(ch_f_out, ch_f_in, ch_send.at[1], ch_recv.at[1], me + size)

    @pl.when(at_group < groups - 1)
    def _():
        to_before.wait_recv()

    @pl.when(at_group == groups - 1)
    def _():
        ch_b_in[...] = jnp.zeros_like(ch_b_in)

    incoming = ch_b_in[0:1]
    above = ch_b_in[1:2]
    ch_b_out[...] = packed(times_t(whole[...], column(incoming)) + y, above + group_stats)

    @pl.when(at_group > 0)
    def _():
        to_before.start()

    for e in range(size - 1, 0, -1):
        new = vec_b[e, 0:1] + times_t(group[e], column(incoming))
        incoming = jnp.where(place < e, new, incoming)

    incoming_c = column(incoming)
    for k in range(sections):
        back[k:k + 1] = times_t(suf[k], incoming_c) + back_local[k:k + 1]
    before = back[...]
    after = jnp.concatenate([before[1:], incoming], axis=0)
    acc = jnp.zeros((nu, LANES), F32)
    for k in range(sections):
        acc = jnp.where(lane_u == k, times(b[k], after[k:k + 1]), acc)
    pulled = turned(acc)[:sections]
    held = grad_input + pulled
    acc = jnp.zeros((nu, LANES), F32)
    for k in range(sections):
        gain = -times(gi[k], held[k:k + 1])
        acc = jnp.where(lane_u == k, gain, acc)
        pushes[k:k + 1] = times_t(b[k], gain)
    forward_gain = turned(acc)[:sections]

    acc = jnp.zeros((ns, ns), F32)
    for k in range(sections):
        drive = -defect[k:k + 1]
        if k:
            drive = drive + pushes[k - 1:k]
        acc = acc + suf[k] * drive
    ended = row_of(jnp.sum(acc, axis=1, keepdims=True)) + pushes[sections - 1:]
    vec_f[pl.ds(place, 1)] = packed(ended, stats)[None]
    f_copies = [
        remote(vec_f.at[place], vec_f.at[place], f_send.at[j], f_recv.at[j], mate)
        for j, mate in enumerate(mates)
    ]
    for copy in f_copies:
        copy.start()

    def forward_alone():
        step = -defect[0:1]
        acc = jnp.where(lane == 0, column(step), 0.0)
        for k in range(1, sections):
            moved = times(m[k - 1], step)
            step = row_of(moved) + pushes[k - 1:k] - defect[k:k + 1]
            acc = jnp.where(lane == k, column(step), acc)
        cols[...] = acc

    @pl.when(at_group > 0)
    def _():
        forward_alone()

    arrive(vec_f, f_send, f_recv)
    y = vec_f[0, 0:1]
    for e in range(1, size):
        y = vec_f[e, 0:1] + row_of(times(group[e], y))

    @pl.when(at_group > 0)
    def _():
        to_after.wait_recv()

    @pl.when(at_group == 0)
    def _():
        ch_f_in[...] = jnp.zeros_like(ch_f_in)

    entering = ch_f_in[0:1]
    below = ch_f_in[1:2]
    ch_f_out[...] = packed(row_of(times(whole[...], entering)) + y, below + group_stats)

    @pl.when(at_group < groups - 1)
    def _():
        to_after.start()

    @pl.when(at_group == 0)
    def _():
        forward_alone()

    for e in range(size - 1):
        new = vec_f[e, 0:1] + row_of(times(group[e], entering))
        entering = jnp.where(place > e, new, entering)

    acc = cols[...] + jnp.where(lane == 0, column(entering), 0.0)
    for k in range(1, sections):
        acc = acc + jnp.where(lane == k, times(pre[k - 1], entering), 0.0)
    state_step = acc.T[:sections]
    packed_out[0:sections] = state_step
    moved = acc[:, :sections] - defect_t
    for k in range(sections):
        packed_out[sections + k:sections + k + 1] = times_t(v[k], moved[:, k:k + 1]) + back[k:k + 1]
    acc = jnp.zeros((nu, LANES), F32)
    for k in range(sections):
        acc = jnp.where(lane_u == k, times(fb[k], state_step[k:k + 1]), acc)
    fed = turned(acc)[:sections]
    chosen = ac[...].astype(F32)
    input_step = (1.0 - chosen) * (fed + forward_gain) + chosen * (ub[...] - inp[...])
    bound_step = chosen * (
        held + jnp.dot(input_step, w[...], precision=PRECISE, preferred_element_type=F32)
    )
    packed_out[2 * sections:3 * sections] = jnp.concatenate(
        [input_step, bound_step, jnp.zeros((sections, ns - 2 * nu), F32)], axis=1
    )
    totals = above + group_stats + below
    tops = totals[:, 0:3]
    scale = totals[:, 3:6]
    spot = lax.broadcasted_iota(jnp.int32, (1, 3), 1)
    horizon = sections * n
    entries = jnp.where(spot == 0, ns, jnp.where(spot == 1, ns + nu, nu)).astype(F32)
    norms = jnp.sqrt(tops / (scale + floor_share * horizon * entries))
    packed_out[3 * sections:3 * sections + 1, 0:3] = norms

    @pl.when(me > 0)
    def _():
        to_earlier.wait_send()

    @pl.when(me < n - 1)
    def _():
        to_later.wait_send()

    for copy in p_copies + b_copies + f_copies:
        copy.wait_send()

    @pl.when(at_group > 0)
    def _():
        to_before.wait_send()

    @pl.when(at_group < groups - 1)
    def _():
        to_after.wait_send()


def spread(sections, ns, nu, packed, o_state, o_input, o_mult, o_bound, o_norm):
    o_state[...] = packed[0:sections]
    o_mult[...] = packed[sections:2 * sections]
    o_input[...] = packed[2 * sections:3 * sections, 0:nu]
    o_bound[...] = packed[2 * sections:3 * sections, nu:2 * nu]
    o_norm[...] = packed[3 * sections:3 * sections + 1, 0:3]


def local(n, *args):
    size = 4 if n % 4 == 0 else (2 if n % 2 == 0 else 1)
    sections, ns = args[12].shape
    nu = args[13].shape[1]
    mates = size - 1
    copies = [pltpu.VMEM(x.shape, x.dtype) for x in args]
    message = (8, ns)
    dma = pltpu.SemaphoreType.DMA
    scratch = copies + [
        pltpu.VMEM((sections, ns, ns), F32),
        pltpu.VMEM((sections, ns, ns), F32),
        pltpu.VMEM((size, ns, ns), F32),
        pltpu.VMEM((ns, ns), F32),
        pltpu.VMEM((sections, ns), F32),
        pltpu.VMEM((sections, ns), F32),
        pltpu.VMEM((sections, ns), F32),
        pltpu.VMEM((sections, ns), F32),
        pltpu.VMEM((sections, ns), F32),
        pltpu.VMEM((ns, LANES), F32),
    ] + [pltpu.VMEM(message, F32)] * 4 + [
        pltpu.VMEM((size,) + message, F32),
        pltpu.VMEM((size,) + message, F32),
    ] + [pltpu.VMEM(message, F32)] * 4 + [
        dma((16,)), dma((sections,)), dma((2,)), dma((2,)),
        dma((4,)), dma((4,)), dma((mates,)), dma((mates,)), dma((mates,)), dma((mates,)),
        dma((2,)), dma((2,)),
    ]
    args = [pltpu.with_memory_space_constraint(x, pltpu.HBM) for x in args]
    packed = pl.pallas_call(
        functools.partial(kernel, n, size),
        out_shape=jax.ShapeDtypeStruct((3 * sections + 8, ns), F32),
        in_specs=[pl.BlockSpec(memory_space=pltpu.HBM)] * len(args),
        out_specs=pl.BlockSpec(memory_space=pltpu.VMEM),
        scratch_shapes=scratch,
        compiler_params=pltpu.CompilerParams(
            collective_id=0, has_side_effects=True, vmem_limit_bytes=VMEM_LIMIT
        ),
    )(*args)
    outs = [(sections, ns), (sections, nu), (sections, ns), (sections, nu), (1, 3)]
    results = pl.pallas_call(
        functools.partial(spread, sections, ns, nu),
        out_shape=[jax.ShapeDtypeStruct(shape, F32) for shape in outs],
        in_specs=[pl.BlockSpec(memory_space=pltpu.VMEM)],
        out_specs=[pl.BlockSpec(memory_space=pltpu.VMEM)] * len(outs),
        compiler_params=pltpu.CompilerParams(vmem_limit_bytes=4 * 1024 * 1024),
    )(packed)
    return (*results[:4], results[4][0])


def solution(mesh):
    wide = P(("batch", "tm"), None, None)
    flat = P(("batch", "tm"), None)
    in_specs = (wide,) * 6 + (P("batch", None),) + (flat,) * 10
    out_specs = (flat,) * 4 + (P("batch"),)
    return jax.shard_map(
        functools.partial(local, mesh.shape["tm"]),
        mesh=mesh, in_specs=in_specs, out_specs=out_specs, check_vma=False,
    )
```

```python
import functools
import jax
import jax.numpy as jnp
from jax import lax
from jax.experimental import pallas as pl
from jax.experimental.pallas import tpu as pltpu
from jax.sharding import PartitionSpec as P

F32 = jnp.float32
BF16 = jnp.bfloat16
PRECISE = lax.Precision.HIGHEST
MESH = pl.DeviceIdType.MESH
floor_share = 0.001
LANES = 128
VMEM_LIMIT = 48 * 1024 * 1024


def parts_of(x):
    high = x.astype(BF16)
    return high, (x - high.astype(F32)).astype(BF16)


def matmul(a, b):
    ah, al = parts_of(a)
    bh, bl = parts_of(b)
    dot = functools.partial(jnp.dot, preferred_element_type=F32)
    return dot(ah, bh) + (dot(ah, bl) + dot(al, bh))


def turned(x):
    rows, cols = x.shape
    up = -rows % LANES
    side = -cols % LANES
    if up:
        x = jnp.concatenate([x, jnp.zeros((up, cols), F32)], axis=0)
    if side:
        x = jnp.concatenate([x, jnp.zeros((rows + up, side), F32)], axis=1)
    return x.T[:cols, :rows]


def column(row):
    return jnp.broadcast_to(row, (LANES, row.shape[1])).T[:, :1]


def row_of(col):
    return jnp.broadcast_to(col, (col.shape[0], LANES)).T[:1]


def times(matrix, row):
    return jnp.sum(matrix * row, axis=1, keepdims=True)


def times_t(matrix, col):
    return jnp.sum(matrix * col, axis=0, keepdims=True)


def column_block(row):
    return jnp.broadcast_to(row, (LANES, row.shape[1])).T


def lift(matrix, block):
    cols = matrix.shape[1]
    parts = [
        jnp.sum(matrix[:, j:j + LANES] * block[:, :min(LANES, cols - j)], axis=0, keepdims=True)
        for j in range(0, cols, LANES)
    ]
    return jnp.concatenate(parts, axis=1) if len(parts) > 1 else parts[0]


def kernel(n, size, *refs):
    (a_hbm, b_hbm, m_hbm, k_hbm, v_hbm, gi_hbm, w_hbm, sw_hbm, sl_hbm, il_hbm, of_hbm, ub_hbm,
     st_hbm, in_hbm, mu_hbm, bm_hbm, ac_hbm,
     packed_out,
     a, b, m, fb, v, gi, w, sw, sl, il, of, ub, st, inp, mu, bm, ac,
     pre, suf, group, heads, tails, turned_w, turned_r,
     sources, pushes, back_local, back, cols,
     fol_in, prd_in, prd_out, fol_out, vec_b, vec_f, direct_in, direct_out,
     ch_b_in, ch_f_in, ch_b_out, ch_f_out,
     load_sem, m_sem, nb_send, nb_recv, p_send, p_recv, b_send, b_recv, f_send, f_recv,
     d_send, d_recv, ch_send, ch_recv) = refs
    me = lax.axis_index("tm")
    place = lax.rem(me, size)
    base = me - place
    at_group = lax.div(me, size)
    groups = n // size
    sections, ns = st.shape
    nu = inp.shape[1]
    half = sections // 2
    last = sections - 1
    first_group, top_group = at_group == 0, at_group == groups - 1

    early = [(st_hbm, st), (in_hbm, inp), (mu_hbm, mu),
             (a_hbm.at[last], a.at[last]), (b_hbm.at[last], b.at[last])]
    small = [(w_hbm, w), (sw_hbm, sw), (sl_hbm, sl), (il_hbm, il), (of_hbm, of), (ub_hbm, ub),
             (bm_hbm, bm), (ac_hbm, ac)]
    rest = pl.ds(0, last)
    large = [(a_hbm.at[rest], a.at[rest]), (b_hbm.at[rest], b.at[rest]), (v_hbm, v), (k_hbm, fb),
             (gi_hbm, gi)]
    loads = [
        pltpu.make_async_copy(src, dst, load_sem.at[i])
        for i, (src, dst) in enumerate(early + small + large)
    ]
    m_loads = [pltpu.make_async_copy(m_hbm.at[k], m.at[k], m_sem.at[k]) for k in range(sections)]
    for i in range(half):
        m_loads[i].start()
        m_loads[half + i].start()
    for load in loads[:len(early)]:
        load.start()

    barrier = pltpu.get_barrier_semaphore()
    mates = [base + lax.rem(place + j, size) for j in range(1, size)]

    def greet(peer):
        pl.semaphore_signal(barrier, inc=1, device_id={"tm": peer}, device_id_type=MESH)

    for mate in mates:
        greet(mate)
    for has, start in ((jnp.logical_not(first_group), base - size),
                       (jnp.logical_not(top_group), base + size)):
        @pl.when(has)
        def _():
            for j in range(size):
                greet(start + j)

    def remote(src, dst, send, recv, peer):
        return pltpu.make_async_remote_copy(
            src_ref=src, dst_ref=dst, send_sem=send, recv_sem=recv,
            device_id={"tm": peer}, device_id_type=MESH,
        )

    for load in loads[:len(early)]:
        load.wait()
    m_loads[0].wait()
    m_loads[half].wait()
    for load in loads[len(early):]:
        load.start()
    for k in range(1, half):
        m_loads[k].wait()
        m_loads[half + k].wait()

    fol_out[...] = mu[0:1]
    moved = row_of(times(a[last], st[last:]))
    prd_out[...] = moved + lift(b[last], column_block(
        jnp.concatenate([inp[last:], jnp.zeros((1, LANES - nu), F32)], axis=1))[:nu])

    lines = [[m.at[k] for k in range(half)], [m.at[k] for k in range(half, sections)]]
    temps = [[suf.at[i] for i in range(half)], [pre.at[half + i] for i in range(half)]]
    ends = [pre.at[half - 1], suf.at[half]]
    while len(lines[0]) > 1:
        grown = [[], []]
        for i in range(0, len(lines[0]) - 1, 2):
            for side, line in enumerate(lines):
                dst = ends[side] if len(line) == 2 else temps[side].pop(0)
                dst[...] = matmul(line[i + 1][...], line[i][...])
                grown[side].append(dst)
        if len(lines[0]) % 2:
            for side, line in enumerate(lines):
                grown[side].append(line[-1])
        lines = grown

    peers = size - 1 + jnp.where(first_group, 0, size) + jnp.where(top_group, 0, size)
    pl.semaphore_wait(barrier, peers)
    to_earlier = remote(fol_out, fol_in, nb_send.at[0], nb_recv.at[0], me - 1)
    to_later = remote(prd_out, prd_in, nb_send.at[1], nb_recv.at[1], me + 1)

    @pl.when(me > 0)
    def _():
        to_earlier.start()

    @pl.when(me < n - 1)
    def _():
        to_later.start()

    along = place + 1 - 2 * lax.rem(place, 2)
    across = place + 2 - 4 * lax.div(place, 2)
    far = size - 1 - place
    top, bottom = pl.ds(0, ns // 2), pl.ds(ns // 2, ns // 2)

    def piece(slot, rows, j, peer):
        ref = group.at[slot, rows]
        return remote(ref, ref, p_send.at[j], p_recv.at[j], base + peer)

    product = matmul(suf[half], pre[half - 1])
    group[pl.ds(place, 1)] = product[None]
    if size == 4:
        p_copies = [piece(place, top, 0, along), piece(place, bottom, 2, across),
                    piece(place, bottom, 1, along), piece(place, top, 3, across)]
    else:
        p_copies = [
            remote(group.at[place], group.at[place], p_send.at[j], p_recv.at[j],
                   base + lax.rem(place + j + 1, size))
            for j in range(size - 1)
        ]
    for copy in p_copies:
        copy.start()
    suf[0] = product

    pre[0] = m[0]
    suf[last] = m[last]
    pre[half] = matmul(m[half], pre[half - 1])
    suf[half - 1] = matmul(suf[half], m[half - 1])

    def grow(i):
        pre[half + i] = matmul(m[half + i], pre[half + i - 1])
        suf[half - 1 - i] = matmul(suf[half - i], m[half - 1 - i])
        pre[i] = matmul(m[i], pre[i - 1])
        suf[last - i] = matmul(suf[sections - i], m[last - i])

    split = half // 2

    @pl.loop(1, split)
    def _(i):
        grow(i)

    for load in loads[len(early):]:
        load.wait()
    lane = lax.broadcasted_iota(jnp.int32, (ns, LANES), 1)
    lane_u = lax.broadcasted_iota(jnp.int32, (nu, LANES), 1)

    inputs_t = turned(inp[...])
    acc = jnp.zeros((ns, LANES), F32)
    for k in range(sections):
        acc = jnp.where(lane == k, times(a[k], st[k:k + 1]), acc)
    predicted = acc.T[:sections]
    rows = [times_t(b[k], inputs_t[:, k:k + 1]) for k in range(sections)]
    predicted = predicted + jnp.concatenate(rows, axis=0)

    @pl.when(me < n - 1)
    def _():
        to_earlier.wait_recv()

    @pl.when(me == n - 1)
    def _():
        fol_in[...] = jnp.zeros_like(fol_in)

    following = jnp.concatenate([mu[1:], fol_in[...]], axis=0)
    following_t = turned(following)
    grad_input = (
        jnp.dot(inp[...], w[...], precision=PRECISE, preferred_element_type=F32) + il[...] + bm[...]
    )
    acc = jnp.zeros((nu, LANES), F32)
    for k in range(sections):
        acc = jnp.where(lane_u == k, times(b[k], following[k:k + 1]), acc)
    grad_input = grad_input - turned(acc)[:sections]
    grad_input_t = turned(grad_input)
    rows = [times_t(a[k], following_t[:, k:k + 1]) for k in range(sections)]
    grad_state = sw[...] * st[...] + sl[...] + mu[...] - jnp.concatenate(rows, axis=0)

    @pl.when(me > 0)
    def _():
        to_later.wait_recv()

    @pl.when(me == 0)
    def _():
        prd_in[...] = jnp.zeros_like(prd_in)

    previous = jnp.concatenate([prd_in[...], predicted[:last]], axis=0)
    defect = st[...] - previous - of[...]
    defect_t = turned(defect)
    rows = [
        times_t(v[k], defect_t[:, k:k + 1]) + times_t(fb[k], grad_input_t[:, k:k + 1])
        for k in range(sections)
    ]
    sources[...] = jnp.concatenate(rows, axis=0) + grad_state
    slack = bm[...] * (ub[...] - inp[...])

    if size == 4:
        piece(along, top, 0, along).wait_recv()
        relays = [piece(along, top, 4, across), piece(across, bottom, 5, along)]
        relays[0].start()
        piece(across, bottom, 2, across).wait_recv()
        relays[1].start()
        p_copies = p_copies + relays

    def total(*xs):
        return sum(
            jnp.sum(jnp.sum(x * x, axis=1, keepdims=True), axis=0, keepdims=True) for x in xs
        )

    sums = [total(defect), total(grad_state, grad_input), total(slack), total(of[...]),
            total(sl[...], il[...]), total(bm[...])]
    line = lax.broadcasted_iota(jnp.int32, (1, ns), 1)
    stats = jnp.zeros((1, ns), F32)
    for i, value in enumerate(sums):
        stats = jnp.where(line == i, value, stats)

    def packed(vector, extra):
        return jnp.concatenate([vector, extra], axis=0)

    costate = sources[last:]
    back_local[last:] = costate
    for k in range(last - 1, -1, -1):
        costate = lift(m[k], column_block(costate)) + sources[k:k + 1]
        back_local[k:k + 1] = costate
    vec_b[pl.ds(place, 1)] = packed(costate, stats)[None]
    b_copies = [
        remote(vec_b.at[place], vec_b.at[place], b_send.at[j], b_recv.at[j], mate)
        for j, mate in enumerate(mates)
    ]
    for copy in b_copies:
        copy.start()

    @pl.loop(split, half - 1)
    def _(i):
        grow(i)

    def arrive(buffer, send, recv):
        for j in range(size - 1):
            source = base + lax.rem(place + size - 1 - j, size)
            slot = source - base
            remote(buffer.at[slot], buffer.at[slot], send.at[j], recv.at[j], source).wait_recv()

    arrive(vec_b, b_send, b_recv)
    if size == 4:
        piece(along, bottom, 1, along).wait_recv()
        piece(across, top, 3, across).wait_recv()
        piece(far, top, 4, across).wait_recv()
        piece(far, bottom, 5, along).wait_recv()
    else:
        arrive(group, p_send, p_recv)
    group_stats = jnp.sum(vec_b[:, 1, :], axis=0, keepdims=True)

    held_in = jnp.zeros((1, ns), F32)
    y = vec_b[size - 1, 0:1]
    for e in range(size - 2, -1, -1):
        held_in = jnp.where(place == e, y, held_in)
        y = vec_b[e, 0:1] + lift(group[e], column_block(y))
    to_before = remote(ch_b_out, ch_b_in, ch_send.at[0], ch_recv.at[0], me - size)
    to_after = remote(ch_f_out, ch_f_in, ch_send.at[1], ch_recv.at[1], me + size)

    @pl.when(top_group)
    def _():
        ch_b_in[...] = jnp.zeros_like(ch_b_in)
        ch_b_out[...] = packed(y, group_stats)

    @pl.when(jnp.logical_and(top_group, jnp.logical_not(first_group)))
    def _():
        to_before.start()

    unit = (lax.broadcasted_iota(jnp.int32, (ns, ns), 0)
            == lax.broadcasted_iota(jnp.int32, (ns, ns), 1)).astype(F32)
    heads[0] = unit
    tails[size - 1] = unit
    for e in range(1, size):
        heads[e] = group[0] if e == 1 else matmul(group[e - 1], heads[e - 1])
        f = size - 1 - e
        tails[f] = group[size - 1] if e == 1 else matmul(tails[f + 1], group[f + 1])
    whole = matmul(group[size - 1], heads[size - 1]) if size > 1 else group[0]
    heads[size] = whole

    for k in range(1, last, 2):
        m[k] = m[k].T

    @pl.when(jnp.logical_not(top_group))
    def _():
        to_before.wait_recv()
        ch_b_out[...] = packed(
            y + lift(heads[size], column_block(ch_b_in[0:1])), ch_b_in[1:2] + group_stats
        )

    @pl.when(jnp.logical_not(jnp.logical_or(top_group, first_group)))
    def _():
        to_before.start()

    above = ch_b_in[1:2]
    incoming = held_in + lift(tails[place], column_block(ch_b_in[0:1]))
    incoming_c = column_block(incoming)
    for k in range(sections):
        back[k:k + 1] = lift(suf[k], incoming_c) + back_local[k:k + 1]
    before = back[...]
    after = jnp.concatenate([before[1:], incoming], axis=0)
    acc = jnp.zeros((nu, LANES), F32)
    for k in range(sections):
        acc = jnp.where(lane_u == k, times(b[k], after[k:k + 1]), acc)
    pulled = turned(acc)[:sections]
    held = grad_input + pulled
    acc = jnp.zeros((nu, LANES), F32)
    for k in range(sections):
        gain = -times(gi[k], held[k:k + 1])
        acc = jnp.where(lane_u == k, gain, acc)
        pushes[k:k + 1] = times_t(b[k], gain)
    forward_gain = turned(acc)[:sections]

    acc = jnp.zeros((ns, ns), F32)
    for k in range(sections):
        drive = -defect[k:k + 1]
        if k:
            drive = drive + pushes[k - 1:k]
        acc = acc + suf[k] * drive
    ended = row_of(jnp.sum(acc, axis=1, keepdims=True)) + pushes[last:]
    vec_f[pl.ds(place, 1)] = ended[None]
    f_copies = [
        remote(vec_f.at[place], vec_f.at[place], f_send.at[j], f_recv.at[j], mate)
        for j, mate in enumerate(mates)
    ]
    direct = [
        remote(direct_out, direct_in.at[place], d_send.at[j], d_recv.at[place], base + size + j)
        for j in range(size)
    ]
    sends_direct = jnp.logical_and(first_group, jnp.logical_not(top_group))

    @pl.when(sends_direct)
    def _():
        direct_out[...] = packed(row_of(times(tails[place], ended)), group_stats)
        for copy in direct:
            copy.start()

    for copy in f_copies:
        copy.start()
    turned_w[...] = heads[size].T
    turned_r[...] = heads[place].T

    drive = jnp.concatenate([jnp.zeros((1, ns), F32), pushes[:last]], axis=0) - defect
    drive_t = turned(drive)
    step = drive[0:1]
    kept = [step]
    acc = jnp.zeros((ns, LANES), F32)
    for k in range(1, sections):
        if k % 2:
            block = jnp.broadcast_to(times(m[k - 1], step), (ns, LANES)) + drive_t[:, k:k + 1]
            acc = jnp.where(lane == k, block, acc)
            kept.append(jnp.zeros((1, ns), F32))
        else:
            step = lift(m[k - 1], block) + drive[k:k + 1]
            kept.append(step)
    kept.append(jnp.zeros((LANES - sections, ns), F32))
    cols[...] = acc + jnp.concatenate(kept, axis=0).T

    arrive(vec_f, f_send, f_recv)
    held_on = jnp.zeros((1, ns), F32)
    y = vec_f[0]
    for e in range(1, size):
        held_on = jnp.where(place == e, y, held_on)
        y = vec_f[e] + row_of(times(group[e], y))

    @pl.when(first_group)
    def _():
        ch_f_in[...] = jnp.zeros_like(ch_f_in)

    @pl.when(at_group == 1)
    def _():
        came = jnp.zeros((1, ns), F32)
        for j in range(size):
            remote(direct_out, direct_in.at[j], d_send.at[j], d_recv.at[j],
                   base - size + j).wait_recv()
            came = came + direct_in[j, 0:1]
        ch_f_in[...] = packed(came, direct_in[0, 1:2])

    @pl.when(at_group > 1)
    def _():
        to_after.wait_recv()

    below = ch_f_in[1:2]
    entering_c = column_block(ch_f_in[0:1])
    goes_on = jnp.logical_and(jnp.logical_not(first_group), jnp.logical_not(top_group))

    @pl.when(goes_on)
    def _():
        ch_f_out[...] = packed(y + lift(turned_w[...], entering_c), below + group_stats)
        to_after.start()

    entering = held_on + lift(turned_r[...], entering_c)

    acc = cols[...] + jnp.where(lane == 0, column(entering), 0.0)
    for k in range(1, sections):
        acc = acc + jnp.where(lane == k, times(pre[k - 1], entering), 0.0)
    state_step = acc.T[:sections]
    packed_out[0:sections] = state_step
    moved = acc[:, :sections] - defect_t
    for k in range(sections):
        packed_out[sections + k:sections + k + 1] = times_t(v[k], moved[:, k:k + 1]) + back[k:k + 1]
    acc = jnp.zeros((nu, LANES), F32)
    for k in range(sections):
        acc = jnp.where(lane_u == k, times(fb[k], state_step[k:k + 1]), acc)
    fed = turned(acc)[:sections]
    chosen = ac[...].astype(F32)
    input_step = (1.0 - chosen) * (fed + forward_gain) + chosen * (ub[...] - inp[...])
    bound_step = chosen * (
        held + jnp.dot(input_step, w[...], precision=PRECISE, preferred_element_type=F32)
    )
    packed_out[2 * sections:3 * sections] = jnp.concatenate(
        [input_step, bound_step, jnp.zeros((sections, ns - 2 * nu), F32)], axis=1
    )
    totals = above + group_stats + below
    tops = totals[:, 0:3]
    scale = totals[:, 3:6]
    spot = lax.broadcasted_iota(jnp.int32, (1, 3), 1)
    horizon = sections * n
    entries = jnp.where(spot == 0, ns, jnp.where(spot == 1, ns + nu, nu)).astype(F32)
    norms = jnp.sqrt(tops / (scale + floor_share * horizon * entries))
    packed_out[3 * sections:3 * sections + 1, 0:3] = norms

    @pl.when(me > 0)
    def _():
        to_earlier.wait_send()

    @pl.when(me < n - 1)
    def _():
        to_later.wait_send()

    for copy in p_copies + b_copies + f_copies:
        copy.wait_send()

    @pl.when(jnp.logical_not(first_group))
    def _():
        to_before.wait_send()

    @pl.when(sends_direct)
    def _():
        for copy in direct:
            copy.wait_send()

    @pl.when(goes_on)
    def _():
        to_after.wait_send()


def spread(sections, ns, nu, packed, o_state, o_input, o_mult, o_bound, o_norm):
    o_state[...] = packed[0:sections]
    o_mult[...] = packed[sections:2 * sections]
    o_input[...] = packed[2 * sections:3 * sections, 0:nu]
    o_bound[...] = packed[2 * sections:3 * sections, nu:2 * nu]
    o_norm[...] = packed[3 * sections:3 * sections + 1, 0:3]


def local(n, *args):
    size = 4 if n % 4 == 0 else (2 if n % 2 == 0 else 1)
    sections, ns = args[12].shape
    nu = args[13].shape[1]
    mates = size - 1
    copies = [pltpu.VMEM(x.shape, x.dtype) for x in args]
    dma = pltpu.SemaphoreType.DMA
    scratch = copies + [
        pltpu.VMEM((sections, ns, ns), F32),
        pltpu.VMEM((sections, ns, ns), F32),
        pltpu.VMEM((size, ns, ns), F32),
        pltpu.VMEM((size + 1, ns, ns), F32),
        pltpu.VMEM((size, ns, ns), F32),
        pltpu.VMEM((ns, ns), F32),
        pltpu.VMEM((ns, ns), F32),
        pltpu.VMEM((sections, ns), F32),
        pltpu.VMEM((sections, ns), F32),
        pltpu.VMEM((sections, ns), F32),
        pltpu.VMEM((sections, ns), F32),
        pltpu.VMEM((ns, LANES), F32),
    ] + [pltpu.VMEM((1, ns), F32)] * 4 + [
        pltpu.VMEM((size, 2, ns), F32),
        pltpu.VMEM((size, 1, ns), F32),
        pltpu.VMEM((size, 2, ns), F32),
    ] + [pltpu.VMEM((2, ns), F32)] * 5 + [
        dma((18,)), dma((sections,)), dma((2,)), dma((2,)),
        dma((6,)), dma((6,)), dma((mates,)), dma((mates,)), dma((mates,)), dma((mates,)),
        dma((size,)), dma((size,)), dma((2,)), dma((2,)),
    ]
    args = [pltpu.with_memory_space_constraint(x, pltpu.HBM) for x in args]
    packed = pl.pallas_call(
        functools.partial(kernel, n, size),
        out_shape=jax.ShapeDtypeStruct((3 * sections + 8, ns), F32),
        in_specs=[pl.BlockSpec(memory_space=pltpu.HBM)] * len(args),
        out_specs=pl.BlockSpec(memory_space=pltpu.VMEM),
        scratch_shapes=scratch,
        compiler_params=pltpu.CompilerParams(
            collective_id=0, has_side_effects=True, vmem_limit_bytes=VMEM_LIMIT
        ),
    )(*args)
    outs = [(sections, ns), (sections, nu), (sections, ns), (sections, nu), (1, 3)]
    results = pl.pallas_call(
        functools.partial(spread, sections, ns, nu),
        out_shape=[jax.ShapeDtypeStruct(shape, F32) for shape in outs],
        in_specs=[pl.BlockSpec(memory_space=pltpu.VMEM)],
        out_specs=[pl.BlockSpec(memory_space=pltpu.VMEM)] * len(outs),
        compiler_params=pltpu.CompilerParams(vmem_limit_bytes=4 * 1024 * 1024),
    )(packed)
    return (*results[:4], results[4][0])


def solution(mesh):
    wide = P(("batch", "tm"), None, None)
    flat = P(("batch", "tm"), None)
    in_specs = (wide,) * 6 + (P("batch", None),) + (flat,) * 10
    out_specs = (flat,) * 4 + (P("batch"),)
    return jax.shard_map(
        functools.partial(local, mesh.shape["tm"]),
        mesh=mesh, in_specs=in_specs, out_specs=out_specs, check_vma=False,
    )
```

```python
import functools
import jax
import jax.numpy as jnp
from jax import lax
from jax.experimental import pallas as pl
from jax.experimental.pallas import tpu as pltpu
from jax.sharding import PartitionSpec as P

F32 = jnp.float32
BF16 = jnp.bfloat16
PRECISE = lax.Precision.HIGHEST
MESH = pl.DeviceIdType.MESH
floor_share = 0.001
LANES = 128
VMEM_LIMIT = 48 * 1024 * 1024


def parts_of(x):
    high = x.astype(BF16)
    return high, (x - high.astype(F32)).astype(BF16)


def matmul(a, b):
    ah, al = parts_of(a)
    bh, bl = parts_of(b)
    dot = functools.partial(jnp.dot, preferred_element_type=F32)
    return dot(ah, bh) + (dot(ah, bl) + dot(al, bh))


def matmul_nt(a, b):
    ah, al = parts_of(a)
    bh, bl = parts_of(b)

    def dot(x, y):
        return lax.dot_general(x, y, (((1,), (1,)), ((), ())), preferred_element_type=F32)

    return dot(ah, bh) + (dot(ah, bl) + dot(al, bh))


def turned(x):
    rows, cols = x.shape
    up = -rows % LANES
    side = -cols % LANES
    if up:
        x = jnp.concatenate([x, jnp.zeros((up, cols), F32)], axis=0)
    if side:
        x = jnp.concatenate([x, jnp.zeros((rows + up, side), F32)], axis=1)
    return x.T[:cols, :rows]


def column(row):
    return jnp.broadcast_to(row, (LANES, row.shape[1])).T[:, :1]


def row_of(col):
    return jnp.broadcast_to(col, (col.shape[0], LANES)).T[:1]


def times(matrix, row):
    return jnp.sum(matrix * row, axis=1, keepdims=True)


def times_t(matrix, col):
    return jnp.sum(matrix * col, axis=0, keepdims=True)


def column_block(row):
    return jnp.broadcast_to(row, (LANES, row.shape[1])).T


def lift(matrix, block):
    cols = matrix.shape[1]
    parts = [
        jnp.sum(matrix[:, j:j + LANES] * block[:, :min(LANES, cols - j)], axis=0, keepdims=True)
        for j in range(0, cols, LANES)
    ]
    return jnp.concatenate(parts, axis=1) if len(parts) > 1 else parts[0]


def kernel(n, size, *refs):
    (a_hbm, b_hbm, m_hbm, k_hbm, v_hbm, gi_hbm, w_hbm, sw_hbm, sl_hbm, il_hbm, of_hbm, ub_hbm,
     st_hbm, in_hbm, mu_hbm, bm_hbm, ac_hbm,
     packed_out,
     a, b, m, fb, v, gi, w, sw, sl, il, of, ub, st, inp, mu, bm, ac,
     pre, suf, group, heads, tails, turned_w, turned_r,
     hess, slope, spread_u, spread_g, fb_t, fed_local, settled,
     sources, pushes, back_local, back, cols,
     fol_in, prd_in, prd_out, fol_out, vec_b, vec_f, direct_in, direct_out,
     ch_b_in, ch_f_in, ch_b_out, ch_f_out, skip_in, skip_w, skip_g, own_g,
     load_sem, m_sem, nb_send, nb_recv, p_send, p_recv, b_send, b_recv, f_send, f_recv,
     d_send, d_recv, ch_send, ch_recv, r_send, r_recv) = refs
    me = lax.axis_index("tm")
    place = lax.rem(me, size)
    base = me - place
    at_group = lax.div(me, size)
    groups = n // size
    sections, ns = st.shape
    nu = inp.shape[1]
    half = sections // 2
    last = sections - 1
    first_group, top_group = at_group == 0, at_group == groups - 1
    relayed = groups == 4
    to_skip = jnp.logical_and(relayed, at_group == 1)
    to_top = jnp.logical_and(relayed, at_group == 2)
    skipped = jnp.logical_and(relayed, at_group == 3)

    early = [(st_hbm, st), (in_hbm, inp), (mu_hbm, mu),
             (a_hbm.at[last], a.at[last]), (b_hbm.at[last], b.at[last])]
    small = [(w_hbm, w), (sw_hbm, sw), (sl_hbm, sl), (il_hbm, il), (of_hbm, of), (ub_hbm, ub),
             (bm_hbm, bm), (ac_hbm, ac)]
    rest = pl.ds(0, last)
    large = [(a_hbm.at[rest], a.at[rest]), (b_hbm.at[rest], b.at[rest]), (v_hbm, v), (k_hbm, fb),
             (gi_hbm, gi)]
    loads = [
        pltpu.make_async_copy(src, dst, load_sem.at[i])
        for i, (src, dst) in enumerate(early + small + large)
    ]
    m_loads = [pltpu.make_async_copy(m_hbm.at[k], m.at[k], m_sem.at[k]) for k in range(sections)]
    for i in range(half):
        m_loads[i].start()
        m_loads[half + i].start()
    for load in loads[:len(early)]:
        load.start()

    barrier = pltpu.get_barrier_semaphore()
    mates = [base + lax.rem(place + j, size) for j in range(1, size)]

    def greet(peer):
        pl.semaphore_signal(barrier, inc=1, device_id={"tm": peer}, device_id_type=MESH)

    for mate in mates:
        greet(mate)
    for has, start in ((jnp.logical_not(first_group), base - size),
                       (jnp.logical_not(top_group), base + size)):
        @pl.when(has)
        def _():
            for j in range(size):
                greet(start + j)

    if relayed:
        for has, peer in ((to_skip, me + 2 * size), (skipped, me - 2 * size)):
            @pl.when(has)
            def _():
                greet(peer)

    def remote(src, dst, send, recv, peer):
        return pltpu.make_async_remote_copy(
            src_ref=src, dst_ref=dst, send_sem=send, recv_sem=recv,
            device_id={"tm": peer}, device_id_type=MESH,
        )

    for load in loads[:len(early)]:
        load.wait()
    m_loads[0].wait()
    m_loads[half].wait()
    for load in loads[len(early):]:
        load.start()
    for k in range(1, half):
        m_loads[k].wait()
        m_loads[half + k].wait()

    fol_out[...] = mu[0:1]
    moved = row_of(times(a[last], st[last:]))
    prd_out[...] = moved + lift(b[last], column_block(
        jnp.concatenate([inp[last:], jnp.zeros((1, LANES - nu), F32)], axis=1))[:nu])

    lines = [[m.at[k] for k in range(half)], [m.at[k] for k in range(half, sections)]]
    temps = [[suf.at[i] for i in range(half)], [pre.at[half + i] for i in range(half)]]
    ends = [pre.at[half - 1], suf.at[half]]
    while len(lines[0]) > 1:
        grown = [[], []]
        for i in range(0, len(lines[0]) - 1, 2):
            for side, line in enumerate(lines):
                dst = ends[side] if len(line) == 2 else temps[side].pop(0)
                dst[...] = matmul(line[i + 1][...], line[i][...])
                grown[side].append(dst)
        if len(lines[0]) % 2:
            for side, line in enumerate(lines):
                grown[side].append(line[-1])
        lines = grown

    peers = size - 1 + jnp.where(first_group, 0, size) + jnp.where(top_group, 0, size)
    peers = peers + jnp.where(jnp.logical_or(to_skip, skipped), 1, 0)
    pl.semaphore_wait(barrier, peers)
    to_earlier = remote(fol_out, fol_in, nb_send.at[0], nb_recv.at[0], me - 1)
    to_later = remote(prd_out, prd_in, nb_send.at[1], nb_recv.at[1], me + 1)

    @pl.when(me > 0)
    def _():
        to_earlier.start()

    @pl.when(me < n - 1)
    def _():
        to_later.start()

    along = place + 1 - 2 * lax.rem(place, 2)
    across = place + 2 - 4 * lax.div(place, 2)
    far = size - 1 - place
    top, bottom = pl.ds(0, ns // 2), pl.ds(ns // 2, ns // 2)

    def piece(slot, rows, j, peer):
        ref = group.at[slot, rows]
        return remote(ref, ref, p_send.at[j], p_recv.at[j], base + peer)

    product = matmul(suf[half], pre[half - 1])
    group[pl.ds(place, 1)] = product[None]
    if size == 4:
        p_copies = [piece(place, top, 0, along), piece(place, bottom, 2, across),
                    piece(place, bottom, 1, along), piece(place, top, 3, across)]
    else:
        p_copies = [
            remote(group.at[place], group.at[place], p_send.at[j], p_recv.at[j],
                   base + lax.rem(place + j + 1, size))
            for j in range(size - 1)
        ]
    for copy in p_copies:
        copy.start()
    suf[0] = product

    pre[0] = m[0]
    suf[last] = m[last]
    pre[half] = matmul(m[half], pre[half - 1])
    suf[half - 1] = matmul(suf[half], m[half - 1])

    def grow(i):
        pre[half + i] = matmul(m[half + i], pre[half + i - 1])
        suf[half - 1 - i] = matmul(suf[half - i], m[half - 1 - i])
        pre[i] = matmul(m[i], pre[i - 1])
        suf[last - i] = matmul(suf[sections - i], m[last - i])

    split = half // 2

    @pl.loop(1, split)
    def _(i):
        grow(i)

    for load in loads[len(early):]:
        load.wait()
    lane = lax.broadcasted_iota(jnp.int32, (ns, LANES), 1)
    lane_u = lax.broadcasted_iota(jnp.int32, (nu, LANES), 1)

    inputs_t = turned(inp[...])
    acc = jnp.zeros((ns, LANES), F32)
    for k in range(sections):
        acc = jnp.where(lane == k, times(a[k], st[k:k + 1]), acc)
    predicted = acc.T[:sections]
    rows = [times_t(b[k], inputs_t[:, k:k + 1]) for k in range(sections)]
    predicted = predicted + jnp.concatenate(rows, axis=0)

    @pl.when(me < n - 1)
    def _():
        to_earlier.wait_recv()

    @pl.when(me == n - 1)
    def _():
        fol_in[...] = jnp.zeros_like(fol_in)

    following = jnp.concatenate([mu[1:], fol_in[...]], axis=0)
    following_t = turned(following)
    grad_input = (
        jnp.dot(inp[...], w[...], precision=PRECISE, preferred_element_type=F32) + il[...] + bm[...]
    )
    acc = jnp.zeros((nu, LANES), F32)
    for k in range(sections):
        acc = jnp.where(lane_u == k, times(b[k], following[k:k + 1]), acc)
    grad_input = grad_input - turned(acc)[:sections]
    grad_input_t = turned(grad_input)
    rows = [times_t(a[k], following_t[:, k:k + 1]) for k in range(sections)]
    grad_state = sw[...] * st[...] + sl[...] + mu[...] - jnp.concatenate(rows, axis=0)

    @pl.when(me > 0)
    def _():
        to_later.wait_recv()

    @pl.when(me == 0)
    def _():
        prd_in[...] = jnp.zeros_like(prd_in)

    previous = jnp.concatenate([prd_in[...], predicted[:last]], axis=0)
    defect = st[...] - previous - of[...]
    defect_t = turned(defect)
    rows = [
        times_t(v[k], defect_t[:, k:k + 1]) + times_t(fb[k], grad_input_t[:, k:k + 1])
        for k in range(sections)
    ]
    sources[...] = jnp.concatenate(rows, axis=0) + grad_state
    slack = bm[...] * (ub[...] - inp[...])

    if size == 4:
        piece(along, top, 0, along).wait_recv()
        relays = [piece(along, top, 4, across), piece(across, bottom, 5, along)]
        relays[0].start()
        piece(across, bottom, 2, across).wait_recv()
        relays[1].start()
        p_copies = p_copies + relays

    def total(*xs):
        return sum(
            jnp.sum(jnp.sum(x * x, axis=1, keepdims=True), axis=0, keepdims=True) for x in xs
        )

    sums = [total(defect), total(grad_state, grad_input), total(slack), total(of[...]),
            total(sl[...], il[...]), total(bm[...])]
    line = lax.broadcasted_iota(jnp.int32, (1, ns), 1)
    stats = jnp.zeros((1, ns), F32)
    for i, value in enumerate(sums):
        stats = jnp.where(line == i, value, stats)

    def packed(vector, extra):
        return jnp.concatenate([vector, extra], axis=0)

    costate = sources[last:]
    back_local[last:] = costate
    for k in range(last - 1, -1, -1):
        costate = lift(m[k], column_block(costate)) + sources[k:k + 1]
        back_local[k:k + 1] = costate
    vec_b[pl.ds(place, 1)] = packed(costate, stats)[None]
    b_copies = [
        remote(vec_b.at[place], vec_b.at[place], b_send.at[j], b_recv.at[j], mate)
        for j, mate in enumerate(mates)
    ]
    for copy in b_copies:
        copy.start()

    @pl.loop(split, half - 1)
    def _(i):
        grow(i)

    def arrive(buffer, send, recv):
        for j in range(size - 1):
            source = base + lax.rem(place + size - 1 - j, size)
            slot = source - base
            remote(buffer.at[slot], buffer.at[slot], send.at[j], recv.at[j], source).wait_recv()

    for k in range(sections):
        fb_t[k] = turned(fb[k])
    sends_direct = jnp.logical_and(first_group, jnp.logical_not(top_group))

    @pl.when(sends_direct)
    def _():
        spread_u[last * nu:] = b[last]
        spread_g[last * nu:] = matmul(gi[last], b[last])
        stride = 5 if last % 5 == 0 else 1

        @pl.loop(0, last // stride)
        def _(i):
            for j in range(stride):
                k = i * stride + j
                u = matmul_nt(b[k], suf[k + 1])
                rows = pl.ds(pl.multiple_of(k * nu, nu), nu)
                spread_u[rows] = u
                spread_g[rows] = matmul(gi[k], u)

        step = ns if (sections * nu) % ns == 0 else nu
        total_h = jnp.zeros((ns, ns), F32)
        for q in range(0, sections * nu, step):
            total_h = total_h + matmul(spread_u[q:q + step].T, spread_g[q:q + step])
        hess[...] = -total_h

    arrive(vec_b, b_send, b_recv)
    if size == 4:
        piece(along, bottom, 1, along).wait_recv()
        piece(across, top, 3, across).wait_recv()
        piece(far, top, 4, across).wait_recv()
        piece(far, bottom, 5, along).wait_recv()
    else:
        arrive(group, p_send, p_recv)
    group_stats = jnp.sum(vec_b[:, 1, :], axis=0, keepdims=True)

    held_in = jnp.zeros((1, ns), F32)
    y = vec_b[size - 1, 0:1]
    for e in range(size - 2, -1, -1):
        held_in = jnp.where(place == e, y, held_in)
        y = vec_b[e, 0:1] + lift(group[e], column_block(y))
    to_before = remote(ch_b_out, ch_b_in, ch_send.at[0], ch_recv.at[0], me - size)
    to_after = remote(ch_f_out, ch_f_in, ch_send.at[1], ch_recv.at[1], me + size)

    @pl.when(top_group)
    def _():
        ch_b_in[...] = jnp.zeros_like(ch_b_in)
        ch_b_out[...] = packed(y, group_stats)

    @pl.when(jnp.logical_and(top_group, jnp.logical_not(first_group)))
    def _():
        to_before.start()

    unit = (lax.broadcasted_iota(jnp.int32, (ns, ns), 0)
            == lax.broadcasted_iota(jnp.int32, (ns, ns), 1)).astype(F32)
    heads[0] = unit
    tails[size - 1] = unit
    for e in range(1, size):
        heads[e] = group[0] if e == 1 else matmul(group[e - 1], heads[e - 1])
        f = size - 1 - e
        tails[f] = group[size - 1] if e == 1 else matmul(tails[f + 1], group[f + 1])
    whole = matmul(group[size - 1], heads[size - 1]) if size > 1 else group[0]
    heads[size] = whole
    turned_w[...] = whole.T
    up_w = remote(turned_w, skip_w, r_send.at[1], r_recv.at[1], me + size)
    up_g = remote(own_g, skip_g, r_send.at[2], r_recv.at[2], me + size)
    up_skip = remote(ch_f_out, skip_in, r_send.at[0], r_recv.at[0], me + 2 * size)

    @pl.when(to_top)
    def _():
        up_w.start()

    for k in range(1, last, 2):
        m[k] = m[k].T

    def middle(incoming):
        incoming_c = column_block(incoming)
        for k in range(sections):
            back[k:k + 1] = lift(suf[k], incoming_c) + back_local[k:k + 1]
        after = jnp.concatenate([back[1:], incoming], axis=0)
        acc = jnp.zeros((nu, LANES), F32)
        for k in range(sections):
            acc = jnp.where(lane_u == k, times(b[k], after[k:k + 1]), acc)
        held = grad_input + turned(acc)[:sections]
        acc = jnp.zeros((nu, LANES), F32)
        for k in range(sections):
            gain = -times(gi[k], held[k:k + 1])
            acc = jnp.where(lane_u == k, gain, acc)
            pushes[k:k + 1] = times_t(b[k], gain)
        forward_gain = turned(acc)[:sections]
        return held, forward_gain

    def end_term():
        acc = jnp.zeros((ns, ns), F32)
        for k in range(sections):
            drive = -defect[k:k + 1]
            if k:
                drive = drive + pushes[k - 1:k]
            acc = acc + suf[k] * drive
        return row_of(jnp.sum(acc, axis=1, keepdims=True)) + pushes[last:]

    direct = [
        remote(direct_out, direct_in.at[place], d_send.at[j], d_recv.at[place], base + size + j)
        for j in range(size)
    ]

    @pl.when(sends_direct)
    def _():
        slope[...] = matmul(tails[place], hess[...])
        middle(held_in)
        ended = end_term()
        settled[...] = packed(ended, row_of(times(tails[place], ended)))
        hess[...] = matmul_nt(slope[...], tails[place])

    @pl.when(jnp.logical_not(top_group))
    def _():
        to_before.wait_recv()
        ch_b_out[...] = packed(
            y + lift(heads[size], column_block(ch_b_in[0:1])), ch_b_in[1:2] + group_stats
        )

    @pl.when(jnp.logical_not(jnp.logical_or(top_group, first_group)))
    def _():
        to_before.start()

    above = ch_b_in[1:2]
    coming_c = column_block(ch_b_in[0:1])

    f_copies = [
        remote(vec_f.at[place], vec_f.at[place], f_send.at[j], f_recv.at[j], mate)
        for j, mate in enumerate(mates)
    ]

    @pl.when(sends_direct)
    def _():
        direct_out[...] = packed(settled[1:2] + lift(hess[...], coming_c), group_stats)
        for copy in direct:
            copy.start()
        vec_f[pl.ds(place, 1)] = (settled[0:1] + lift(slope[...], coming_c))[None]
        for copy in f_copies:
            copy.start()

    held, forward_gain = middle(held_in + lift(tails[place], coming_c))

    @pl.when(jnp.logical_not(sends_direct))
    def _():
        vec_f[pl.ds(place, 1)] = end_term()[None]
        for copy in f_copies:
            copy.start()

    turned_r[...] = heads[place].T

    drive = jnp.concatenate([jnp.zeros((1, ns), F32), pushes[:last]], axis=0) - defect
    drive_t = turned(drive)
    step = drive[0:1]
    kept = [step]
    acc = jnp.zeros((ns, LANES), F32)
    for k in range(1, sections):
        if k % 2:
            block = jnp.broadcast_to(times(m[k - 1], step), (ns, LANES)) + drive_t[:, k:k + 1]
            acc = jnp.where(lane == k, block, acc)
            kept.append(jnp.zeros((1, ns), F32))
        else:
            step = lift(m[k - 1], block) + drive[k:k + 1]
            kept.append(step)
    kept.append(jnp.zeros((LANES - sections, ns), F32))
    cols[...] = acc + jnp.concatenate(kept, axis=0).T

    moved = cols[:, :sections] - defect_t
    acc = jnp.zeros((nu, LANES), F32)
    alone = cols[...].T
    for k in range(sections):
        packed_out[sections + k:sections + k + 1] = times_t(v[k], moved[:, k:k + 1]) + back[k:k + 1]
        acc = jnp.where(lane_u == k, times(fb[k], alone[k:k + 1]), acc)
    fed_local[...] = turned(acc)[:sections]

    arrive(vec_f, f_send, f_recv)
    held_on = jnp.zeros((1, ns), F32)
    y = vec_f[0]
    for e in range(1, size):
        held_on = jnp.where(place == e, y, held_on)
        y = vec_f[e] + row_of(times(group[e], y))

    @pl.when(first_group)
    def _():
        ch_f_in[...] = jnp.zeros_like(ch_f_in)

    @pl.when(at_group == 1)
    def _():
        came = jnp.zeros((1, ns), F32)
        for j in range(size):
            remote(direct_out, direct_in.at[j], d_send.at[j], d_recv.at[j],
                   base - size + j).wait_recv()
            came = came + direct_in[j, 0:1]
        ch_f_in[...] = packed(came, direct_in[0, 1:2])

    @pl.when(to_top)
    def _():
        own_g[...] = packed(y, group_stats)
        up_g.start()

    @pl.when(jnp.logical_and(at_group > 1, jnp.logical_not(skipped)))
    def _():
        to_after.wait_recv()

    @pl.when(skipped)
    def _():
        up_w.wait_recv()
        up_g.wait_recv()
        up_skip.wait_recv()
        ch_f_in[...] = packed(
            skip_g[0:1] + lift(skip_w[...], column_block(skip_in[0:1])), skip_g[1:2] + skip_in[1:2]
        )

    below = ch_f_in[1:2]
    entering_c = column_block(ch_f_in[0:1])
    goes_on = jnp.logical_not(jnp.logical_or(jnp.logical_or(first_group, top_group), to_top))

    @pl.when(goes_on)
    def _():
        ch_f_out[...] = packed(y + lift(turned_w[...], entering_c), below + group_stats)
        to_after.start()

    @pl.when(to_skip)
    def _():
        up_skip.start()

    entering = held_on + lift(turned_r[...], entering_c)

    acc = cols[...]
    fed = []
    for k in range(sections):
        if k:
            block = jnp.broadcast_to(times(pre[k - 1], entering), (ns, LANES))
        else:
            block = column_block(entering)
        acc = acc + jnp.where(lane == k, block, 0.0)
        packed_out[sections + k:sections + k + 1] = (
            packed_out[sections + k:sections + k + 1] + lift(v[k], block)
        )
        fed.append(lift(fb_t[k], block))
    packed_out[0:sections] = acc.T[:sections]
    fed = jnp.concatenate(fed, axis=0) + fed_local[...]
    chosen = ac[...].astype(F32)
    input_step = (1.0 - chosen) * (fed + forward_gain) + chosen * (ub[...] - inp[...])
    bound_step = chosen * (
        held + jnp.dot(input_step, w[...], precision=PRECISE, preferred_element_type=F32)
    )
    packed_out[2 * sections:3 * sections] = jnp.concatenate(
        [input_step, bound_step, jnp.zeros((sections, ns - 2 * nu), F32)], axis=1
    )
    totals = above + group_stats + below
    tops = totals[:, 0:3]
    scale = totals[:, 3:6]
    spot = lax.broadcasted_iota(jnp.int32, (1, 3), 1)
    horizon = sections * n
    entries = jnp.where(spot == 0, ns, jnp.where(spot == 1, ns + nu, nu)).astype(F32)
    norms = jnp.sqrt(tops / (scale + floor_share * horizon * entries))
    packed_out[3 * sections:3 * sections + 1, 0:3] = norms

    @pl.when(me > 0)
    def _():
        to_earlier.wait_send()

    @pl.when(me < n - 1)
    def _():
        to_later.wait_send()

    for copy in p_copies + b_copies + f_copies:
        copy.wait_send()

    @pl.when(jnp.logical_not(first_group))
    def _():
        to_before.wait_send()

    @pl.when(sends_direct)
    def _():
        for copy in direct:
            copy.wait_send()

    @pl.when(goes_on)
    def _():
        to_after.wait_send()

    @pl.when(to_skip)
    def _():
        up_skip.wait_send()

    @pl.when(to_top)
    def _():
        up_w.wait_send()
        up_g.wait_send()


def spread(sections, ns, nu, packed, o_state, o_input, o_mult, o_bound, o_norm):
    o_state[...] = packed[0:sections]
    o_mult[...] = packed[sections:2 * sections]
    o_input[...] = packed[2 * sections:3 * sections, 0:nu]
    o_bound[...] = packed[2 * sections:3 * sections, nu:2 * nu]
    o_norm[...] = packed[3 * sections:3 * sections + 1, 0:3]


def local(n, *args):
    size = 4 if n % 4 == 0 else (2 if n % 2 == 0 else 1)
    sections, ns = args[12].shape
    nu = args[13].shape[1]
    mates = size - 1
    copies = [pltpu.VMEM(x.shape, x.dtype) for x in args]
    dma = pltpu.SemaphoreType.DMA
    scratch = copies + [
        pltpu.VMEM((sections, ns, ns), F32),
        pltpu.VMEM((sections, ns, ns), F32),
        pltpu.VMEM((size, ns, ns), F32),
        pltpu.VMEM((size + 1, ns, ns), F32),
        pltpu.VMEM((size, ns, ns), F32),
        pltpu.VMEM((ns, ns), F32),
        pltpu.VMEM((ns, ns), F32),
        pltpu.VMEM((ns, ns), F32),
        pltpu.VMEM((ns, ns), F32),
        pltpu.VMEM((sections * nu, ns), F32),
        pltpu.VMEM((sections * nu, ns), F32),
        pltpu.VMEM((sections, ns, nu), F32),
        pltpu.VMEM((sections, nu), F32),
        pltpu.VMEM((2, ns), F32),
        pltpu.VMEM((sections, ns), F32),
        pltpu.VMEM((sections, ns), F32),
        pltpu.VMEM((sections, ns), F32),
        pltpu.VMEM((sections, ns), F32),
        pltpu.VMEM((ns, LANES), F32),
    ] + [pltpu.VMEM((1, ns), F32)] * 4 + [
        pltpu.VMEM((size, 2, ns), F32),
        pltpu.VMEM((size, 1, ns), F32),
        pltpu.VMEM((size, 2, ns), F32),
    ] + [pltpu.VMEM((2, ns), F32)] * 6 + [
        pltpu.VMEM((ns, ns), F32), pltpu.VMEM((2, ns), F32), pltpu.VMEM((2, ns), F32),
        dma((18,)), dma((sections,)), dma((2,)), dma((2,)),
        dma((6,)), dma((6,)), dma((mates,)), dma((mates,)), dma((mates,)), dma((mates,)),
        dma((size,)), dma((size,)), dma((2,)), dma((2,)), dma((3,)), dma((3,)),
    ]
    args = [pltpu.with_memory_space_constraint(x, pltpu.HBM) for x in args]
    packed = pl.pallas_call(
        functools.partial(kernel, n, size),
        out_shape=jax.ShapeDtypeStruct((3 * sections + 8, ns), F32),
        in_specs=[pl.BlockSpec(memory_space=pltpu.HBM)] * len(args),
        out_specs=pl.BlockSpec(memory_space=pltpu.VMEM),
        scratch_shapes=scratch,
        compiler_params=pltpu.CompilerParams(
            collective_id=0, has_side_effects=True, vmem_limit_bytes=VMEM_LIMIT
        ),
    )(*args)
    outs = [(sections, ns), (sections, nu), (sections, ns), (sections, nu), (1, 3)]
    results = pl.pallas_call(
        functools.partial(spread, sections, ns, nu),
        out_shape=[jax.ShapeDtypeStruct(shape, F32) for shape in outs],
        in_specs=[pl.BlockSpec(memory_space=pltpu.VMEM)],
        out_specs=[pl.BlockSpec(memory_space=pltpu.VMEM)] * len(outs),
        compiler_params=pltpu.CompilerParams(vmem_limit_bytes=4 * 1024 * 1024),
    )(packed)
    return (*results[:4], results[4][0])


def solution(mesh):
    wide = P(("batch", "tm"), None, None)
    flat = P(("batch", "tm"), None)
    in_specs = (wide,) * 6 + (P("batch", None),) + (flat,) * 10
    out_specs = (flat,) * 4 + (P("batch"),)
    return jax.shard_map(
        functools.partial(local, mesh.shape["tm"]),
        mesh=mesh, in_specs=in_specs, out_specs=out_specs, check_vma=False,
    )
```

```python
import functools
import jax
import jax.numpy as jnp
from jax import lax
from jax.experimental import pallas as pl
from jax.experimental.pallas import tpu as pltpu
from jax.sharding import PartitionSpec as P

F32 = jnp.float32
BF16 = jnp.bfloat16
PRECISE = lax.Precision.HIGHEST
MESH = pl.DeviceIdType.MESH
floor_share = 0.001
LANES = 128
VMEM_LIMIT = 48 * 1024 * 1024


def parts_of(x):
    high = x.astype(BF16)
    return high, (x - high.astype(F32)).astype(BF16)


def matmul(a, b):
    ah, al = parts_of(a)
    bh, bl = parts_of(b)
    dot = functools.partial(jnp.dot, preferred_element_type=F32)
    return dot(ah, bh) + (dot(ah, bl) + dot(al, bh))


def matmul_nt(a, b):
    ah, al = parts_of(a)
    bh, bl = parts_of(b)

    def dot(x, y):
        return lax.dot_general(x, y, (((1,), (1,)), ((), ())), preferred_element_type=F32)

    return dot(ah, bh) + (dot(ah, bl) + dot(al, bh))


def turned(x):
    rows, cols = x.shape
    up = -rows % LANES
    side = -cols % LANES
    if up:
        x = jnp.concatenate([x, jnp.zeros((up, cols), F32)], axis=0)
    if side:
        x = jnp.concatenate([x, jnp.zeros((rows + up, side), F32)], axis=1)
    return x.T[:cols, :rows]


def column(row):
    return jnp.broadcast_to(row, (LANES, row.shape[1])).T[:, :1]


def row_of(col):
    return jnp.broadcast_to(col, (col.shape[0], LANES)).T[:1]


def times(matrix, row):
    return jnp.sum(matrix * row, axis=1, keepdims=True)


def times_t(matrix, col):
    return jnp.sum(matrix * col, axis=0, keepdims=True)


def column_block(row):
    return jnp.broadcast_to(row, (LANES, row.shape[1])).T


def lift(matrix, block):
    cols = matrix.shape[1]
    parts = [
        jnp.sum(matrix[:, j:j + LANES] * block[:, :min(LANES, cols - j)], axis=0, keepdims=True)
        for j in range(0, cols, LANES)
    ]
    return jnp.concatenate(parts, axis=1) if len(parts) > 1 else parts[0]


def kernel(n, size, parts, *refs):
    (a_hbm, b_hbm, m_hbm, k_hbm, v_hbm, gi_hbm, w_hbm, sw_hbm, sl_hbm, il_hbm, of_hbm, ub_hbm,
     st_hbm, in_hbm, mu_hbm, bm_hbm, ac_hbm,
     packed_out,
     a, b, m, fb, v, gi, w, sw, sl, il, of, ub, st, inp, mu, bm, ac,
     pre, suf, group, heads, tails, turned_w, turned_r,
     hess, slope, spread_u, spread_g, fb_t, fed_local, settled,
     sources, pushes, back_local, back, cols,
     fol_in, prd_in, prd_out, fol_out, vec_b, vec_f, direct_in, direct_out,
     ch_b_in, ch_f_in, ch_b_out, ch_f_out, skip_in, skip_w, skip_g, own_g,
     twin_in, twin_out, twin_y, twin_w,
     load_sem, m_sem, nb_send, nb_recv, p_send, p_recv, b_send, b_recv, f_send, f_recv,
     d_send, d_recv, ch_send, ch_recv, r_send, r_recv, t_send, t_recv) = refs
    me = lax.axis_index("tm")
    place = lax.rem(me, size)
    base = me - place
    at_group = lax.div(me, size)
    groups = n // size
    sections, ns = st.shape
    nu = inp.shape[1]
    half = sections // 2
    last = sections - 1
    first_group, top_group = at_group == 0, at_group == groups - 1
    relayed = groups == 4
    paired = parts == 2 and groups > 2
    part = lax.axis_index("batch")
    twin = 1 - part
    serves = jnp.logical_and(paired, part == 1)
    served = jnp.logical_and(paired, part == 0)
    inner_group = jnp.logical_not(jnp.logical_or(first_group, top_group))
    to_skip = jnp.logical_and(relayed, at_group == 1)
    to_top = jnp.logical_and(relayed, at_group == 2)
    skipped = jnp.logical_and(relayed, at_group == 3)

    early = [(st_hbm, st), (in_hbm, inp), (mu_hbm, mu),
             (a_hbm.at[last], a.at[last]), (b_hbm.at[last], b.at[last])]
    small = [(w_hbm, w), (sw_hbm, sw), (sl_hbm, sl), (il_hbm, il), (of_hbm, of), (ub_hbm, ub),
             (bm_hbm, bm), (ac_hbm, ac)]
    rest = pl.ds(0, last)
    large = [(a_hbm.at[rest], a.at[rest]), (b_hbm.at[rest], b.at[rest]), (v_hbm, v), (k_hbm, fb),
             (gi_hbm, gi)]
    loads = [
        pltpu.make_async_copy(src, dst, load_sem.at[i])
        for i, (src, dst) in enumerate(early + small + large)
    ]
    m_loads = [pltpu.make_async_copy(m_hbm.at[k], m.at[k], m_sem.at[k]) for k in range(sections)]
    for i in range(half):
        m_loads[i].start()
        m_loads[half + i].start()
    for load in loads[:len(early)]:
        load.start()

    barrier = pltpu.get_barrier_semaphore()
    mates = [base + lax.rem(place + j, size) for j in range(1, size)]

    def greet(peer):
        pl.semaphore_signal(barrier, inc=1, device_id={"tm": peer}, device_id_type=MESH)

    for mate in mates:
        greet(mate)
    for has, start in ((jnp.logical_not(first_group), base - size),
                       (jnp.logical_not(top_group), base + size)):
        @pl.when(has)
        def _():
            for j in range(size):
                greet(start + j)

    if relayed:
        for has, peer in ((to_skip, me + 2 * size), (skipped, me - 2 * size)):
            @pl.when(has)
            def _():
                greet(peer)

    def greet_twin(peer):
        pl.semaphore_signal(
            barrier, inc=1, device_id={"tm": peer, "batch": twin}, device_id_type=MESH
        )

    if paired:
        greet_twin(me)
        for has, peer in ((jnp.logical_not(first_group), me - size),
                          (jnp.logical_not(top_group), me + size)):
            @pl.when(has)
            def _():
                greet_twin(peer)

    def remote(src, dst, send, recv, peer, other=None):
        device = {"tm": peer} if other is None else {"tm": peer, "batch": other}
        return pltpu.make_async_remote_copy(
            src_ref=src, dst_ref=dst, send_sem=send, recv_sem=recv,
            device_id=device, device_id_type=MESH,
        )

    for load in loads[:len(early)]:
        load.wait()
    m_loads[0].wait()
    m_loads[half].wait()
    for load in loads[len(early):]:
        load.start()
    for k in range(1, half):
        m_loads[k].wait()
        m_loads[half + k].wait()

    fol_out[...] = mu[0:1]
    moved = row_of(times(a[last], st[last:]))
    prd_out[...] = moved + lift(b[last], column_block(
        jnp.concatenate([inp[last:], jnp.zeros((1, LANES - nu), F32)], axis=1))[:nu])

    lines = [[m.at[k] for k in range(half)], [m.at[k] for k in range(half, sections)]]
    temps = [[suf.at[i] for i in range(half)], [pre.at[half + i] for i in range(half)]]
    ends = [pre.at[half - 1], suf.at[half]]
    while len(lines[0]) > 1:
        grown = [[], []]
        for i in range(0, len(lines[0]) - 1, 2):
            for side, line in enumerate(lines):
                dst = ends[side] if len(line) == 2 else temps[side].pop(0)
                dst[...] = matmul(line[i + 1][...], line[i][...])
                grown[side].append(dst)
        if len(lines[0]) % 2:
            for side, line in enumerate(lines):
                grown[side].append(line[-1])
        lines = grown

    peers = size - 1 + jnp.where(first_group, 0, size) + jnp.where(top_group, 0, size)
    peers = peers + jnp.where(jnp.logical_or(to_skip, skipped), 1, 0)
    if paired:
        peers = peers + 1 + jnp.where(first_group, 0, 1) + jnp.where(top_group, 0, 1)
    pl.semaphore_wait(barrier, peers)
    to_earlier = remote(fol_out, fol_in, nb_send.at[0], nb_recv.at[0], me - 1)
    to_later = remote(prd_out, prd_in, nb_send.at[1], nb_recv.at[1], me + 1)

    @pl.when(me > 0)
    def _():
        to_earlier.start()

    @pl.when(me < n - 1)
    def _():
        to_later.start()

    along = place + 1 - 2 * lax.rem(place, 2)
    across = place + 2 - 4 * lax.div(place, 2)
    far = size - 1 - place
    top, bottom = pl.ds(0, ns // 2), pl.ds(ns // 2, ns // 2)

    def piece(slot, rows, j, peer):
        ref = group.at[slot, rows]
        return remote(ref, ref, p_send.at[j], p_recv.at[j], base + peer)

    product = matmul(suf[half], pre[half - 1])
    group[pl.ds(place, 1)] = product[None]
    if size == 4:
        p_copies = [piece(place, top, 0, along), piece(place, bottom, 2, across),
                    piece(place, bottom, 1, along), piece(place, top, 3, across)]
    else:
        p_copies = [
            remote(group.at[place], group.at[place], p_send.at[j], p_recv.at[j],
                   base + lax.rem(place + j + 1, size))
            for j in range(size - 1)
        ]
    for copy in p_copies:
        copy.start()
    suf[0] = product

    pre[0] = m[0]
    suf[last] = m[last]
    pre[half] = matmul(m[half], pre[half - 1])
    suf[half - 1] = matmul(suf[half], m[half - 1])

    def grow(i):
        pre[half + i] = matmul(m[half + i], pre[half + i - 1])
        suf[half - 1 - i] = matmul(suf[half - i], m[half - 1 - i])
        pre[i] = matmul(m[i], pre[i - 1])
        suf[last - i] = matmul(suf[sections - i], m[last - i])

    split = half // 2

    @pl.loop(1, split)
    def _(i):
        grow(i)

    for load in loads[len(early):]:
        load.wait()
    lane = lax.broadcasted_iota(jnp.int32, (ns, LANES), 1)
    lane_u = lax.broadcasted_iota(jnp.int32, (nu, LANES), 1)

    inputs_t = turned(inp[...])
    acc = jnp.zeros((ns, LANES), F32)
    for k in range(sections):
        acc = jnp.where(lane == k, times(a[k], st[k:k + 1]), acc)
    predicted = acc.T[:sections]
    rows = [times_t(b[k], inputs_t[:, k:k + 1]) for k in range(sections)]
    predicted = predicted + jnp.concatenate(rows, axis=0)

    @pl.when(me < n - 1)
    def _():
        to_earlier.wait_recv()

    @pl.when(me == n - 1)
    def _():
        fol_in[...] = jnp.zeros_like(fol_in)

    following = jnp.concatenate([mu[1:], fol_in[...]], axis=0)
    following_t = turned(following)
    grad_input = (
        jnp.dot(inp[...], w[...], precision=PRECISE, preferred_element_type=F32) + il[...] + bm[...]
    )
    acc = jnp.zeros((nu, LANES), F32)
    for k in range(sections):
        acc = jnp.where(lane_u == k, times(b[k], following[k:k + 1]), acc)
    grad_input = grad_input - turned(acc)[:sections]
    grad_input_t = turned(grad_input)
    rows = [times_t(a[k], following_t[:, k:k + 1]) for k in range(sections)]
    grad_state = sw[...] * st[...] + sl[...] + mu[...] - jnp.concatenate(rows, axis=0)

    @pl.when(me > 0)
    def _():
        to_later.wait_recv()

    @pl.when(me == 0)
    def _():
        prd_in[...] = jnp.zeros_like(prd_in)

    previous = jnp.concatenate([prd_in[...], predicted[:last]], axis=0)
    defect = st[...] - previous - of[...]
    defect_t = turned(defect)
    rows = [
        times_t(v[k], defect_t[:, k:k + 1]) + times_t(fb[k], grad_input_t[:, k:k + 1])
        for k in range(sections)
    ]
    sources[...] = jnp.concatenate(rows, axis=0) + grad_state
    slack = bm[...] * (ub[...] - inp[...])

    if size == 4:
        piece(along, top, 0, along).wait_recv()
        relays = [piece(along, top, 4, across), piece(across, bottom, 5, along)]
        relays[0].start()
        piece(across, bottom, 2, across).wait_recv()
        relays[1].start()
        p_copies = p_copies + relays

    def total(*xs):
        return sum(
            jnp.sum(jnp.sum(x * x, axis=1, keepdims=True), axis=0, keepdims=True) for x in xs
        )

    sums = [total(defect), total(grad_state, grad_input), total(slack), total(of[...]),
            total(sl[...], il[...]), total(bm[...])]
    line = lax.broadcasted_iota(jnp.int32, (1, ns), 1)
    stats = jnp.zeros((1, ns), F32)
    for i, value in enumerate(sums):
        stats = jnp.where(line == i, value, stats)

    def packed(vector, extra):
        return jnp.concatenate([vector, extra], axis=0)

    costate = sources[last:]
    back_local[last:] = costate
    for k in range(last - 1, -1, -1):
        costate = lift(m[k], column_block(costate)) + sources[k:k + 1]
        back_local[k:k + 1] = costate
    vec_b[pl.ds(place, 1)] = packed(costate, stats)[None]
    b_copies = [
        remote(vec_b.at[place], vec_b.at[place], b_send.at[j], b_recv.at[j], mate)
        for j, mate in enumerate(mates)
    ]
    for copy in b_copies:
        copy.start()

    @pl.loop(split, half - 1)
    def _(i):
        grow(i)

    def arrive(buffer, send, recv):
        for j in range(size - 1):
            source = base + lax.rem(place + size - 1 - j, size)
            slot = source - base
            remote(buffer.at[slot], buffer.at[slot], send.at[j], recv.at[j], source).wait_recv()

    for k in range(sections):
        fb_t[k] = turned(fb[k])
    sends_direct = jnp.logical_and(first_group, jnp.logical_not(top_group))

    @pl.when(sends_direct)
    def _():
        spread_u[last * nu:] = b[last]
        spread_g[last * nu:] = matmul(gi[last], b[last])
        stride = 15 if last % 15 == 0 else 1

        @pl.loop(0, last // stride)
        def _(i):
            for j in range(stride):
                k = i * stride + j
                u = matmul_nt(b[k], suf[k + 1])
                rows = pl.ds(pl.multiple_of(k * nu, nu), nu)
                spread_u[rows] = u
                spread_g[rows] = matmul(gi[k], u)

        step = ns if (sections * nu) % ns == 0 else nu
        total_h = jnp.zeros((ns, ns), F32)
        for q in range(0, sections * nu, step):
            total_h = total_h + matmul(spread_u[q:q + step].T, spread_g[q:q + step])
        hess[...] = -total_h

    arrive(vec_b, b_send, b_recv)
    if size == 4:
        piece(along, bottom, 1, along).wait_recv()
        piece(across, top, 3, across).wait_recv()
        piece(far, top, 4, across).wait_recv()
        piece(far, bottom, 5, along).wait_recv()
    else:
        arrive(group, p_send, p_recv)
    group_stats = jnp.sum(vec_b[:, 1, :], axis=0, keepdims=True)

    held_in = jnp.zeros((1, ns), F32)
    y = vec_b[size - 1, 0:1]
    for e in range(size - 2, -1, -1):
        held_in = jnp.where(place == e, y, held_in)
        y = vec_b[e, 0:1] + lift(group[e], column_block(y))
    to_before = remote(ch_b_out, ch_b_in, ch_send.at[0], ch_recv.at[0], me - size)
    to_after = remote(ch_f_out, ch_f_in, ch_send.at[1], ch_recv.at[1], me + size)

    @pl.when(top_group)
    def _():
        ch_b_in[...] = jnp.zeros_like(ch_b_in)
        ch_b_out[...] = packed(y, group_stats)

    @pl.when(jnp.logical_and(top_group, jnp.logical_not(first_group)))
    def _():
        to_before.start()

    enter_twin = remote(ch_b_out, twin_in, t_send.at[0], t_recv.at[0], me - size, twin)
    give_y = remote(ch_f_out, twin_y, t_send.at[1], t_recv.at[1], me, twin)
    give_w = remote(heads.at[size], twin_w, t_send.at[2], t_recv.at[2], me, twin)
    pass_on = remote(twin_out, twin_in, t_send.at[0], t_recv.at[0], me - size)
    hand_back = remote(twin_out, ch_b_in, t_send.at[3], ch_recv.at[0], me - size, twin)
    gives = jnp.logical_and(served, inner_group)
    if paired:
        @pl.when(jnp.logical_and(served, top_group))
        def _():
            enter_twin.start()

        @pl.when(gives)
        def _():
            ch_f_out[...] = packed(y, group_stats)
            give_y.start()

    unit = (lax.broadcasted_iota(jnp.int32, (ns, ns), 0)
            == lax.broadcasted_iota(jnp.int32, (ns, ns), 1)).astype(F32)
    heads[0] = unit
    tails[size - 1] = unit
    for e in range(1, size):
        heads[e] = group[0] if e == 1 else matmul(group[e - 1], heads[e - 1])
        f = size - 1 - e
        tails[f] = group[size - 1] if e == 1 else matmul(tails[f + 1], group[f + 1])

    @pl.when(inner_group)
    def _():
        whole = matmul(group[size - 1], heads[size - 1]) if size > 1 else group[0]
        heads[size] = whole
        turned_w[...] = whole.T

    up_w = remote(turned_w, skip_w, r_send.at[1], r_recv.at[1], me + size)
    up_g = remote(own_g, skip_g, r_send.at[2], r_recv.at[2], me + size)
    up_skip = remote(ch_f_out, skip_in, r_send.at[0], r_recv.at[0], me + 2 * size)

    if paired:
        @pl.when(gives)
        def _():
            give_w.start()

    @pl.when(to_top)
    def _():
        up_w.start()

    for k in range(1, last, 2):
        m[k] = m[k].T

    def middle(incoming):
        incoming_c = column_block(incoming)
        for k in range(sections):
            back[k:k + 1] = lift(suf[k], incoming_c) + back_local[k:k + 1]
        after = jnp.concatenate([back[1:], incoming], axis=0)
        acc = jnp.zeros((nu, LANES), F32)
        for k in range(sections):
            acc = jnp.where(lane_u == k, times(b[k], after[k:k + 1]), acc)
        held = grad_input + turned(acc)[:sections]
        acc = jnp.zeros((nu, LANES), F32)
        for k in range(sections):
            gain = -times(gi[k], held[k:k + 1])
            acc = jnp.where(lane_u == k, gain, acc)
            pushes[k:k + 1] = times_t(b[k], gain)
        forward_gain = turned(acc)[:sections]
        return held, forward_gain

    def end_term():
        acc = jnp.zeros((ns, ns), F32)
        for k in range(sections):
            drive = -defect[k:k + 1]
            if k:
                drive = drive + pushes[k - 1:k]
            acc = acc + suf[k] * drive
        return row_of(jnp.sum(acc, axis=1, keepdims=True)) + pushes[last:]

    direct = [
        remote(direct_out, direct_in.at[place], d_send.at[j], d_recv.at[place], base + size + j)
        for j in range(size)
    ]

    @pl.when(sends_direct)
    def _():
        slope[...] = matmul(tails[place], hess[...])
        middle(held_in)
        ended = end_term()
        settled[...] = packed(ended, row_of(times(tails[place], ended)))
        hess[...] = matmul_nt(slope[...], tails[place])

    @pl.when(jnp.logical_not(top_group))
    def _():
        to_before.wait_recv()

    carries = inner_group
    if paired:
        carries = jnp.logical_and(inner_group, jnp.logical_not(served))

    @pl.when(carries)
    def _():
        ch_b_out[...] = packed(
            y + lift(heads[size], column_block(ch_b_in[0:1])), ch_b_in[1:2] + group_stats
        )
        to_before.start()

    helps = jnp.logical_and(serves, inner_group)
    hops_on = jnp.logical_and(helps, at_group > 1)
    if paired:
        @pl.when(helps)
        def _():
            give_y.wait_recv()
            give_w.wait_recv()
            enter_twin.wait_recv()
            twin_out[...] = packed(
                twin_y[0:1] + lift(twin_w[...], column_block(twin_in[0:1])),
                twin_y[1:2] + twin_in[1:2],
            )
            hand_back.start()

        @pl.when(hops_on)
        def _():
            pass_on.start()

        @pl.when(gives)
        def _():
            give_y.wait_send()

    above = ch_b_in[1:2]
    coming_c = column_block(ch_b_in[0:1])

    f_copies = [
        remote(vec_f.at[place], vec_f.at[place], f_send.at[j], f_recv.at[j], mate)
        for j, mate in enumerate(mates)
    ]

    @pl.when(sends_direct)
    def _():
        direct_out[...] = packed(settled[1:2] + lift(hess[...], coming_c), group_stats)
        for copy in direct:
            copy.start()
        vec_f[pl.ds(place, 1)] = (settled[0:1] + lift(slope[...], coming_c))[None]
        for copy in f_copies:
            copy.start()

    held, forward_gain = middle(held_in + lift(tails[place], coming_c))

    @pl.when(jnp.logical_not(sends_direct))
    def _():
        vec_f[pl.ds(place, 1)] = end_term()[None]
        for copy in f_copies:
            copy.start()

    turned_r[...] = heads[place].T

    drive = jnp.concatenate([jnp.zeros((1, ns), F32), pushes[:last]], axis=0) - defect
    drive_t = turned(drive)
    step = drive[0:1]
    kept = [step]
    acc = jnp.zeros((ns, LANES), F32)
    for k in range(1, sections):
        if k % 2:
            block = jnp.broadcast_to(times(m[k - 1], step), (ns, LANES)) + drive_t[:, k:k + 1]
            acc = jnp.where(lane == k, block, acc)
            kept.append(jnp.zeros((1, ns), F32))
        else:
            step = lift(m[k - 1], block) + drive[k:k + 1]
            kept.append(step)
    kept.append(jnp.zeros((LANES - sections, ns), F32))
    cols[...] = acc + jnp.concatenate(kept, axis=0).T

    moved = cols[:, :sections] - defect_t
    acc = jnp.zeros((nu, LANES), F32)
    alone = cols[...].T
    for k in range(sections):
        packed_out[sections + k:sections + k + 1] = times_t(v[k], moved[:, k:k + 1]) + back[k:k + 1]
        acc = jnp.where(lane_u == k, times(fb[k], alone[k:k + 1]), acc)
    fed_local[...] = turned(acc)[:sections]

    arrive(vec_f, f_send, f_recv)
    held_on = jnp.zeros((1, ns), F32)
    y = vec_f[0]
    for e in range(1, size):
        held_on = jnp.where(place == e, y, held_on)
        y = vec_f[e] + row_of(times(group[e], y))

    @pl.when(first_group)
    def _():
        ch_f_in[...] = jnp.zeros_like(ch_f_in)

    @pl.when(at_group == 1)
    def _():
        came = jnp.zeros((1, ns), F32)
        for j in range(size):
            remote(direct_out, direct_in.at[j], d_send.at[j], d_recv.at[j],
                   base - size + j).wait_recv()
            came = came + direct_in[j, 0:1]
        ch_f_in[...] = packed(came, direct_in[0, 1:2])

    @pl.when(to_top)
    def _():
        own_g[...] = packed(y, group_stats)
        up_g.start()

    @pl.when(jnp.logical_and(at_group > 1, jnp.logical_not(skipped)))
    def _():
        to_after.wait_recv()

    @pl.when(skipped)
    def _():
        up_w.wait_recv()
        up_g.wait_recv()
        up_skip.wait_recv()
        ch_f_in[...] = packed(
            skip_g[0:1] + lift(skip_w[...], column_block(skip_in[0:1])), skip_g[1:2] + skip_in[1:2]
        )

    below = ch_f_in[1:2]
    entering_c = column_block(ch_f_in[0:1])
    goes_on = jnp.logical_not(jnp.logical_or(jnp.logical_or(first_group, top_group), to_top))

    @pl.when(goes_on)
    def _():
        ch_f_out[...] = packed(y + lift(turned_w[...], entering_c), below + group_stats)
        to_after.start()

    @pl.when(to_skip)
    def _():
        up_skip.start()

    entering = held_on + lift(turned_r[...], entering_c)

    acc = cols[...]
    fed = []
    for k in range(sections):
        if k:
            block = jnp.broadcast_to(times(pre[k - 1], entering), (ns, LANES))
        else:
            block = column_block(entering)
        acc = acc + jnp.where(lane == k, block, 0.0)
        packed_out[sections + k:sections + k + 1] = (
            packed_out[sections + k:sections + k + 1] + lift(v[k], block)
        )
        fed.append(lift(fb_t[k], block))
    packed_out[0:sections] = acc.T[:sections]
    fed = jnp.concatenate(fed, axis=0) + fed_local[...]
    chosen = ac[...].astype(F32)
    input_step = (1.0 - chosen) * (fed + forward_gain) + chosen * (ub[...] - inp[...])
    bound_step = chosen * (
        held + jnp.dot(input_step, w[...], precision=PRECISE, preferred_element_type=F32)
    )
    packed_out[2 * sections:3 * sections] = jnp.concatenate(
        [input_step, bound_step, jnp.zeros((sections, ns - 2 * nu), F32)], axis=1
    )
    totals = above + group_stats + below
    tops = totals[:, 0:3]
    scale = totals[:, 3:6]
    spot = lax.broadcasted_iota(jnp.int32, (1, 3), 1)
    horizon = sections * n
    entries = jnp.where(spot == 0, ns, jnp.where(spot == 1, ns + nu, nu)).astype(F32)
    norms = jnp.sqrt(tops / (scale + floor_share * horizon * entries))
    packed_out[3 * sections:3 * sections + 1, 0:3] = norms

    @pl.when(me > 0)
    def _():
        to_earlier.wait_send()

    @pl.when(me < n - 1)
    def _():
        to_later.wait_send()

    for copy in p_copies + b_copies + f_copies:
        copy.wait_send()

    @pl.when(jnp.logical_or(jnp.logical_and(top_group, jnp.logical_not(first_group)), carries))
    def _():
        to_before.wait_send()

    if paired:
        @pl.when(jnp.logical_and(served, top_group))
        def _():
            enter_twin.wait_send()

        @pl.when(gives)
        def _():
            give_w.wait_send()

        @pl.when(helps)
        def _():
            hand_back.wait_send()

        @pl.when(hops_on)
        def _():
            pass_on.wait_send()

    @pl.when(sends_direct)
    def _():
        for copy in direct:
            copy.wait_send()

    @pl.when(goes_on)
    def _():
        to_after.wait_send()

    @pl.when(to_skip)
    def _():
        up_skip.wait_send()

    @pl.when(to_top)
    def _():
        up_w.wait_send()
        up_g.wait_send()


def spread(sections, ns, nu, packed, o_state, o_input, o_mult, o_bound, o_norm):
    o_state[...] = packed[0:sections]
    o_mult[...] = packed[sections:2 * sections]
    o_input[...] = packed[2 * sections:3 * sections, 0:nu]
    o_bound[...] = packed[2 * sections:3 * sections, nu:2 * nu]
    o_norm[...] = packed[3 * sections:3 * sections + 1, 0:3]


def local(n, parts, *args):
    size = 4 if n % 4 == 0 else (2 if n % 2 == 0 else 1)
    sections, ns = args[12].shape
    nu = args[13].shape[1]
    mates = size - 1
    copies = [pltpu.VMEM(x.shape, x.dtype) for x in args]
    dma = pltpu.SemaphoreType.DMA
    scratch = copies + [
        pltpu.VMEM((sections, ns, ns), F32),
        pltpu.VMEM((sections, ns, ns), F32),
        pltpu.VMEM((size, ns, ns), F32),
        pltpu.VMEM((size + 1, ns, ns), F32),
        pltpu.VMEM((size, ns, ns), F32),
        pltpu.VMEM((ns, ns), F32),
        pltpu.VMEM((ns, ns), F32),
        pltpu.VMEM((ns, ns), F32),
        pltpu.VMEM((ns, ns), F32),
        pltpu.VMEM((sections * nu, ns), F32),
        pltpu.VMEM((sections * nu, ns), F32),
        pltpu.VMEM((sections, ns, nu), F32),
        pltpu.VMEM((sections, nu), F32),
        pltpu.VMEM((2, ns), F32),
        pltpu.VMEM((sections, ns), F32),
        pltpu.VMEM((sections, ns), F32),
        pltpu.VMEM((sections, ns), F32),
        pltpu.VMEM((sections, ns), F32),
        pltpu.VMEM((ns, LANES), F32),
    ] + [pltpu.VMEM((1, ns), F32)] * 4 + [
        pltpu.VMEM((size, 2, ns), F32),
        pltpu.VMEM((size, 1, ns), F32),
        pltpu.VMEM((size, 2, ns), F32),
    ] + [pltpu.VMEM((2, ns), F32)] * 6 + [
        pltpu.VMEM((ns, ns), F32), pltpu.VMEM((2, ns), F32), pltpu.VMEM((2, ns), F32),
    ] + [pltpu.VMEM((2, ns), F32)] * 3 + [
        pltpu.VMEM((ns, ns), F32),
        dma((18,)), dma((sections,)), dma((2,)), dma((2,)),
        dma((6,)), dma((6,)), dma((mates,)), dma((mates,)), dma((mates,)), dma((mates,)),
        dma((size,)), dma((size,)), dma((2,)), dma((2,)), dma((3,)), dma((3,)), dma((4,)), dma((3,)),
    ]
    args = [pltpu.with_memory_space_constraint(x, pltpu.HBM) for x in args]
    packed = pl.pallas_call(
        functools.partial(kernel, n, size, parts),
        out_shape=jax.ShapeDtypeStruct((3 * sections + 8, ns), F32),
        in_specs=[pl.BlockSpec(memory_space=pltpu.HBM)] * len(args),
        out_specs=pl.BlockSpec(memory_space=pltpu.VMEM),
        scratch_shapes=scratch,
        compiler_params=pltpu.CompilerParams(
            collective_id=0, has_side_effects=True, vmem_limit_bytes=VMEM_LIMIT
        ),
    )(*args)
    outs = [(sections, ns), (sections, nu), (sections, ns), (sections, nu), (1, 3)]
    results = pl.pallas_call(
        functools.partial(spread, sections, ns, nu),
        out_shape=[jax.ShapeDtypeStruct(shape, F32) for shape in outs],
        in_specs=[pl.BlockSpec(memory_space=pltpu.VMEM)],
        out_specs=[pl.BlockSpec(memory_space=pltpu.VMEM)] * len(outs),
        compiler_params=pltpu.CompilerParams(vmem_limit_bytes=4 * 1024 * 1024),
    )(packed)
    return (*results[:4], results[4][0])


def solution(mesh):
    wide = P(("batch", "tm"), None, None)
    flat = P(("batch", "tm"), None)
    in_specs = (wide,) * 6 + (P("batch", None),) + (flat,) * 10
    out_specs = (flat,) * 4 + (P("batch"),)
    return jax.shard_map(
        functools.partial(local, mesh.shape["tm"], mesh.shape["batch"]),
        mesh=mesh, in_specs=in_specs, out_specs=out_specs, check_vma=False,
    )
```

```python
import functools
import jax
import jax.numpy as jnp
from jax import lax
from jax.experimental import pallas as pl
from jax.experimental.pallas import tpu as pltpu
from jax.sharding import PartitionSpec as P

F32 = jnp.float32
BF16 = jnp.bfloat16
PRECISE = lax.Precision.HIGHEST
MESH = pl.DeviceIdType.MESH
floor_share = 0.001
LANES = 128
VMEM_LIMIT = 48 * 1024 * 1024


def parts_of(x):
    high = x.astype(BF16)
    return high, (x - high.astype(F32)).astype(BF16)


def matmul(a, b):
    ah, al = parts_of(a)
    bh, bl = parts_of(b)
    dot = functools.partial(jnp.dot, preferred_element_type=F32)
    return dot(ah, bh) + (dot(ah, bl) + dot(al, bh))


def matmul_nt(a, b):
    ah, al = parts_of(a)
    bh, bl = parts_of(b)

    def dot(x, y):
        return lax.dot_general(x, y, (((1,), (1,)), ((), ())), preferred_element_type=F32)

    return dot(ah, bh) + (dot(ah, bl) + dot(al, bh))


def turned(x):
    rows, cols = x.shape
    up = -rows % LANES
    side = -cols % LANES
    if up:
        x = jnp.concatenate([x, jnp.zeros((up, cols), F32)], axis=0)
    if side:
        x = jnp.concatenate([x, jnp.zeros((rows + up, side), F32)], axis=1)
    return x.T[:cols, :rows]


def column(row):
    return jnp.broadcast_to(row, (LANES, row.shape[1])).T[:, :1]


def row_of(col):
    return jnp.broadcast_to(col, (col.shape[0], LANES)).T[:1]


def times(matrix, row):
    return jnp.sum(matrix * row, axis=1, keepdims=True)


def times_t(matrix, col):
    return jnp.sum(matrix * col, axis=0, keepdims=True)


def column_block(row):
    return jnp.broadcast_to(row, (LANES, row.shape[1])).T


def lift(matrix, block):
    cols = matrix.shape[1]
    parts = [
        jnp.sum(matrix[:, j:j + LANES] * block[:, :min(LANES, cols - j)], axis=0, keepdims=True)
        for j in range(0, cols, LANES)
    ]
    return jnp.concatenate(parts, axis=1) if len(parts) > 1 else parts[0]


def kernel(n, size, parts, *refs):
    (a_hbm, b_hbm, m_hbm, k_hbm, v_hbm, gi_hbm, w_hbm, sw_hbm, sl_hbm, il_hbm, of_hbm, ub_hbm,
     st_hbm, in_hbm, mu_hbm, bm_hbm, ac_hbm,
     packed_out,
     a, b, m, fb, v, gi, w, sw, sl, il, of, ub, st, inp, mu, bm, ac,
     pre, suf, group, heads, tails, turned_w, turned_r,
     hess, slope, spread_u, spread_g, fb_t, fed_local, settled,
     sources, pushes, back_local, back, cols,
     fol_in, prd_in, prd_out, fol_out, vec_b, vec_f, direct_in, direct_out,
     ch_b_in, ch_f_in, ch_b_out, ch_f_out, skip_in, skip_w, skip_g, own_g,
     twin_in, twin_out, twin_y, twin_w, joins,
     load_sem, m_sem, nb_send, nb_recv, p_send, p_recv, b_send, b_recv, f_send, f_recv,
     d_send, d_recv, ch_send, ch_recv, r_send, r_recv, t_send, t_recv) = refs
    me = lax.axis_index("tm")
    place = lax.rem(me, size)
    base = me - place
    at_group = lax.div(me, size)
    groups = n // size
    sections, ns = st.shape
    nu = inp.shape[1]
    half = sections // 2
    last = sections - 1
    first_group, top_group = at_group == 0, at_group == groups - 1
    relayed = groups == 4
    paired = parts == 2 and groups > 2
    part = lax.axis_index("batch")
    twin = 1 - part
    serves = jnp.logical_and(paired, part == 1)
    served = jnp.logical_and(paired, part == 0)
    inner_group = jnp.logical_not(jnp.logical_or(first_group, top_group))
    to_skip = jnp.logical_and(relayed, at_group == 1)
    to_top = jnp.logical_and(relayed, at_group == 2)
    skipped = jnp.logical_and(relayed, at_group == 3)

    early = [(st_hbm, st), (in_hbm, inp), (mu_hbm, mu),
             (a_hbm.at[last], a.at[last]), (b_hbm.at[last], b.at[last])]
    small = [(w_hbm, w), (sw_hbm, sw), (sl_hbm, sl), (il_hbm, il), (of_hbm, of), (ub_hbm, ub),
             (bm_hbm, bm), (ac_hbm, ac)]
    rest = pl.ds(0, last)
    large = [(a_hbm.at[rest], a.at[rest]), (b_hbm.at[rest], b.at[rest]), (v_hbm, v), (k_hbm, fb),
             (gi_hbm, gi)]
    loads = [
        pltpu.make_async_copy(src, dst, load_sem.at[i])
        for i, (src, dst) in enumerate(early + small + large)
    ]
    m_loads = [pltpu.make_async_copy(m_hbm.at[k], m.at[k], m_sem.at[k]) for k in range(sections)]
    for i in range(half):
        m_loads[i].start()
        m_loads[half + i].start()
    for load in loads[:len(early)]:
        load.start()

    barrier = pltpu.get_barrier_semaphore()
    mates = [base + lax.rem(place + j, size) for j in range(1, size)]

    def greet(peer):
        pl.semaphore_signal(barrier, inc=1, device_id={"tm": peer}, device_id_type=MESH)

    for mate in mates:
        greet(mate)
    for has, start in ((jnp.logical_not(first_group), base - size),
                       (jnp.logical_not(top_group), base + size)):
        @pl.when(has)
        def _():
            for j in range(size):
                greet(start + j)

    if relayed:
        for has, peer in ((to_skip, me + 2 * size), (skipped, me - 2 * size)):
            @pl.when(has)
            def _():
                greet(peer)

    def greet_twin(peer):
        pl.semaphore_signal(
            barrier, inc=1, device_id={"tm": peer, "batch": twin}, device_id_type=MESH
        )

    if paired:
        greet_twin(me)
        for has, peer in ((jnp.logical_not(first_group), me - size),
                          (jnp.logical_not(top_group), me + size)):
            @pl.when(has)
            def _():
                greet_twin(peer)

    def remote(src, dst, send, recv, peer, other=None):
        device = {"tm": peer} if other is None else {"tm": peer, "batch": other}
        return pltpu.make_async_remote_copy(
            src_ref=src, dst_ref=dst, send_sem=send, recv_sem=recv,
            device_id=device, device_id_type=MESH,
        )

    for load in loads[:len(early)]:
        load.wait()
    m_loads[0].wait()
    m_loads[half].wait()
    for load in loads[len(early):]:
        load.start()
    for k in range(1, half):
        m_loads[k].wait()
        m_loads[half + k].wait()

    fol_out[...] = mu[0:1]
    moved = row_of(times(a[last], st[last:]))
    prd_out[...] = moved + lift(b[last], column_block(
        jnp.concatenate([inp[last:], jnp.zeros((1, LANES - nu), F32)], axis=1))[:nu])

    lines = [[m.at[k] for k in range(half)], [m.at[k] for k in range(half, sections)]]
    temps = [[suf.at[i] for i in range(half)], [pre.at[half + i] for i in range(half)]]
    ends = [pre.at[half - 1], suf.at[half]]
    while len(lines[0]) > 1:
        grown = [[], []]
        for i in range(0, len(lines[0]) - 1, 2):
            for side, line in enumerate(lines):
                dst = ends[side] if len(line) == 2 else temps[side].pop(0)
                dst[...] = matmul(line[i + 1][...], line[i][...])
                grown[side].append(dst)
        if len(lines[0]) % 2:
            for side, line in enumerate(lines):
                grown[side].append(line[-1])
        lines = grown

    peers = size - 1 + jnp.where(first_group, 0, size) + jnp.where(top_group, 0, size)
    peers = peers + jnp.where(jnp.logical_or(to_skip, skipped), 1, 0)
    if paired:
        peers = peers + 1 + jnp.where(first_group, 0, 1) + jnp.where(top_group, 0, 1)
    pl.semaphore_wait(barrier, peers)
    to_earlier = remote(fol_out, fol_in, nb_send.at[0], nb_recv.at[0], me - 1)
    to_later = remote(prd_out, prd_in, nb_send.at[1], nb_recv.at[1], me + 1)

    @pl.when(me > 0)
    def _():
        to_earlier.start()

    @pl.when(me < n - 1)
    def _():
        to_later.start()

    along = place + 1 - 2 * lax.rem(place, 2)
    across = place + 2 - 4 * lax.div(place, 2)
    far = size - 1 - place
    top, bottom = pl.ds(0, ns // 2), pl.ds(ns // 2, ns // 2)

    def piece(slot, rows, j, peer):
        ref = group.at[slot, rows]
        return remote(ref, ref, p_send.at[j], p_recv.at[j], base + peer)

    product = matmul(suf[half], pre[half - 1])
    group[pl.ds(place, 1)] = product[None]
    if size == 4:
        p_copies = [piece(place, top, 0, along), piece(place, bottom, 2, across),
                    piece(place, bottom, 1, along), piece(place, top, 3, across)]
    else:
        p_copies = [
            remote(group.at[place], group.at[place], p_send.at[j], p_recv.at[j],
                   base + lax.rem(place + j + 1, size))
            for j in range(size - 1)
        ]
    for copy in p_copies:
        copy.start()
    suf[0] = product

    pre[0] = m[0]
    suf[last] = m[last]
    pre[half] = matmul(m[half], pre[half - 1])
    suf[half - 1] = matmul(suf[half], m[half - 1])

    def grow(i):
        pre[half + i] = matmul(m[half + i], pre[half + i - 1])
        suf[half - 1 - i] = matmul(suf[half - i], m[half - 1 - i])
        pre[i] = matmul(m[i], pre[i - 1])
        suf[last - i] = matmul(suf[sections - i], m[last - i])

    split = half // 2

    @pl.loop(1, split)
    def _(i):
        grow(i)

    for load in loads[len(early):]:
        load.wait()
    lane = lax.broadcasted_iota(jnp.int32, (ns, LANES), 1)
    lane_u = lax.broadcasted_iota(jnp.int32, (nu, LANES), 1)

    inputs_t = turned(inp[...])
    acc = jnp.zeros((ns, LANES), F32)
    for k in range(sections):
        acc = jnp.where(lane == k, times(a[k], st[k:k + 1]), acc)
    predicted = acc.T[:sections]
    rows = [times_t(b[k], inputs_t[:, k:k + 1]) for k in range(sections)]
    predicted = predicted + jnp.concatenate(rows, axis=0)

    @pl.when(me < n - 1)
    def _():
        to_earlier.wait_recv()

    @pl.when(me == n - 1)
    def _():
        fol_in[...] = jnp.zeros_like(fol_in)

    following = jnp.concatenate([mu[1:], fol_in[...]], axis=0)
    following_t = turned(following)
    grad_input = (
        jnp.dot(inp[...], w[...], precision=PRECISE, preferred_element_type=F32) + il[...] + bm[...]
    )
    acc = jnp.zeros((nu, LANES), F32)
    for k in range(sections):
        acc = jnp.where(lane_u == k, times(b[k], following[k:k + 1]), acc)
    grad_input = grad_input - turned(acc)[:sections]
    grad_input_t = turned(grad_input)
    rows = [times_t(a[k], following_t[:, k:k + 1]) for k in range(sections)]
    grad_state = sw[...] * st[...] + sl[...] + mu[...] - jnp.concatenate(rows, axis=0)

    @pl.when(me > 0)
    def _():
        to_later.wait_recv()

    @pl.when(me == 0)
    def _():
        prd_in[...] = jnp.zeros_like(prd_in)

    previous = jnp.concatenate([prd_in[...], predicted[:last]], axis=0)
    defect = st[...] - previous - of[...]
    defect_t = turned(defect)
    rows = [
        times_t(v[k], defect_t[:, k:k + 1]) + times_t(fb[k], grad_input_t[:, k:k + 1])
        for k in range(sections)
    ]
    sources[...] = jnp.concatenate(rows, axis=0) + grad_state
    slack = bm[...] * (ub[...] - inp[...])

    if size == 4:
        piece(along, top, 0, along).wait_recv()
        relays = [piece(along, top, 4, across), piece(across, bottom, 5, along)]
        relays[0].start()
        piece(across, bottom, 2, across).wait_recv()
        relays[1].start()
        p_copies = p_copies + relays

    def total(*xs):
        return sum(
            jnp.sum(jnp.sum(x * x, axis=1, keepdims=True), axis=0, keepdims=True) for x in xs
        )

    sums = [total(defect), total(grad_state, grad_input), total(slack), total(of[...]),
            total(sl[...], il[...]), total(bm[...])]
    line = lax.broadcasted_iota(jnp.int32, (1, ns), 1)
    stats = jnp.zeros((1, ns), F32)
    for i, value in enumerate(sums):
        stats = jnp.where(line == i, value, stats)

    def packed(vector, extra):
        return jnp.concatenate([vector, extra], axis=0)

    costate = sources[last:]
    back_local[last:] = costate
    for k in range(last - 1, -1, -1):
        costate = lift(m[k], column_block(costate)) + sources[k:k + 1]
        back_local[k:k + 1] = costate
    vec_b[pl.ds(place, 1)] = packed(costate, stats)[None]
    b_copies = [
        remote(vec_b.at[place], vec_b.at[place], b_send.at[j], b_recv.at[j], mate)
        for j, mate in enumerate(mates)
    ]
    for copy in b_copies:
        copy.start()

    @pl.loop(split, half - 1)
    def _(i):
        grow(i)

    def arrive(buffer, send, recv):
        for j in range(size - 1):
            source = base + lax.rem(place + size - 1 - j, size)
            slot = source - base
            remote(buffer.at[slot], buffer.at[slot], send.at[j], recv.at[j], source).wait_recv()

    @pl.when(jnp.logical_not(first_group))
    def _():
        for k in range(sections):
            fb_t[k] = turned(fb[k])

    sends_direct = jnp.logical_and(first_group, jnp.logical_not(top_group))

    @pl.when(sends_direct)
    def _():
        spread_u[last * nu:] = b[last]
        spread_g[last * nu:] = matmul(gi[last], b[last])
        stride = 15 if last % 15 == 0 else 1

        @pl.loop(0, last // stride)
        def _(i):
            for j in range(stride):
                k = i * stride + j
                u = matmul_nt(b[k], suf[k + 1])
                rows = pl.ds(pl.multiple_of(k * nu, nu), nu)
                spread_u[rows] = u
                spread_g[rows] = matmul(gi[k], u)

        step = ns if (sections * nu) % ns == 0 else nu
        total_h = jnp.zeros((ns, ns), F32)
        for q in range(0, sections * nu, step):
            total_h = total_h + matmul(spread_u[q:q + step].T, spread_g[q:q + step])
        hess[...] = -total_h

    arrive(vec_b, b_send, b_recv)
    if size == 4:
        piece(along, bottom, 1, along).wait_recv()
        piece(across, top, 3, across).wait_recv()
        piece(far, top, 4, across).wait_recv()
        piece(far, bottom, 5, along).wait_recv()
    else:
        arrive(group, p_send, p_recv)
    group_stats = jnp.sum(vec_b[:, 1, :], axis=0, keepdims=True)

    held_in = jnp.zeros((1, ns), F32)
    y = vec_b[size - 1, 0:1]
    for e in range(size - 2, -1, -1):
        held_in = jnp.where(place == e, y, held_in)
        y = vec_b[e, 0:1] + lift(group[e], column_block(y))
    to_before = remote(ch_b_out, ch_b_in, ch_send.at[0], ch_recv.at[0], me - size)
    to_after = remote(ch_f_out, ch_f_in, ch_send.at[1], ch_recv.at[1], me + size)

    @pl.when(top_group)
    def _():
        ch_b_in[...] = jnp.zeros_like(ch_b_in)
        ch_b_out[...] = packed(y, group_stats)

    @pl.when(jnp.logical_and(top_group, jnp.logical_not(first_group)))
    def _():
        to_before.start()

    enter_twin = remote(ch_b_out, twin_in, t_send.at[0], t_recv.at[0], me - size, twin)
    give_y = remote(ch_f_out, twin_y, t_send.at[1], t_recv.at[1], me, twin)
    give_w = remote(heads.at[size], twin_w, t_send.at[2], t_recv.at[2], me, twin)
    pass_on = remote(twin_out, twin_in, t_send.at[0], t_recv.at[0], me - size)
    hand_back = remote(twin_out, ch_b_in, t_send.at[3], ch_recv.at[0], me - size, twin)
    gives = jnp.logical_and(served, inner_group)
    if paired:
        @pl.when(jnp.logical_and(served, top_group))
        def _():
            enter_twin.start()

        @pl.when(gives)
        def _():
            ch_f_out[...] = packed(y, group_stats)
            give_y.start()

    unit = (lax.broadcasted_iota(jnp.int32, (ns, ns), 0)
            == lax.broadcasted_iota(jnp.int32, (ns, ns), 1)).astype(F32)
    heads[0] = unit
    tails[size - 1] = unit

    def widen(e):
        heads[e] = group[0] if e == 1 else matmul(group[e - 1], heads[e - 1])
        f = size - 1 - e
        tails[f] = group[size - 1] if e == 1 else matmul(tails[f + 1], group[f + 1])

    middle_e = size // 2
    for e in range(1, middle_e + 1):
        widen(e)

    @pl.when(inner_group)
    def _():
        heads[size] = matmul(tails[middle_e - 1], heads[middle_e]) if size > 1 else group[0]

    if paired:
        @pl.when(gives)
        def _():
            give_w.start()

    for e in range(middle_e + 1, size):
        widen(e)

    @pl.when(inner_group)
    def _():
        turned_w[...] = heads[size].T

    up_w = remote(turned_w, skip_w, r_send.at[1], r_recv.at[1], me + size)
    up_g = remote(own_g, skip_g, r_send.at[2], r_recv.at[2], me + size)
    up_skip = remote(ch_f_out, skip_in, r_send.at[0], r_recv.at[0], me + 2 * size)

    @pl.when(to_top)
    def _():
        up_w.start()

    for k in range(1, last, 2):
        m[k] = m[k].T

    def middle(incoming):
        incoming_c = column_block(incoming)
        for k in range(sections):
            back[k:k + 1] = lift(suf[k], incoming_c) + back_local[k:k + 1]
        after = jnp.concatenate([back[1:], incoming], axis=0)
        acc = jnp.zeros((nu, LANES), F32)
        for k in range(sections):
            acc = jnp.where(lane_u == k, times(b[k], after[k:k + 1]), acc)
        held = grad_input + turned(acc)[:sections]
        acc = jnp.zeros((nu, LANES), F32)
        for k in range(sections):
            gain = -times(gi[k], held[k:k + 1])
            acc = jnp.where(lane_u == k, gain, acc)
            pushes[k:k + 1] = times_t(b[k], gain)
        forward_gain = turned(acc)[:sections]
        return held, forward_gain

    def end_term():
        acc = jnp.zeros((ns, ns), F32)
        for k in range(sections):
            drive = -defect[k:k + 1]
            if k:
                drive = drive + pushes[k - 1:k]
            acc = acc + suf[k] * drive
        return row_of(jnp.sum(acc, axis=1, keepdims=True)) + pushes[last:]

    direct = [
        remote(direct_out, direct_in.at[place], d_send.at[j], d_recv.at[place], base + size + j)
        for j in range(size)
    ]

    @pl.when(sends_direct)
    def _():
        slope[...] = matmul(tails[place], hess[...])
        middle(held_in)
        ended = end_term()
        settled[...] = packed(ended, row_of(times(tails[place], ended)))
        hess[...] = matmul_nt(slope[...], tails[place])

    @pl.when(jnp.logical_not(top_group))
    def _():
        to_before.wait_recv()

    carries = inner_group
    if paired:
        carries = jnp.logical_and(inner_group, jnp.logical_not(served))

    @pl.when(carries)
    def _():
        ch_b_out[...] = packed(
            y + lift(heads[size], column_block(ch_b_in[0:1])), ch_b_in[1:2] + group_stats
        )
        to_before.start()

    helps = jnp.logical_and(serves, inner_group)
    hops_on = jnp.logical_and(helps, at_group > 1)
    if paired:
        @pl.when(helps)
        def _():
            give_y.wait_recv()
            give_w.wait_recv()
            enter_twin.wait_recv()
            twin_out[...] = packed(
                twin_y[0:1] + lift(twin_w[...], column_block(twin_in[0:1])),
                twin_y[1:2] + twin_in[1:2],
            )
            hand_back.start()

        @pl.when(hops_on)
        def _():
            pass_on.start()

        @pl.when(gives)
        def _():
            give_y.wait_send()

    above = ch_b_in[1:2]
    coming_c = column_block(ch_b_in[0:1])

    f_copies = [
        remote(vec_f.at[place], vec_f.at[place], f_send.at[j], f_recv.at[j], mate)
        for j, mate in enumerate(mates)
    ]

    @pl.when(sends_direct)
    def _():
        direct_out[...] = packed(settled[1:2] + lift(hess[...], coming_c), group_stats)
        for copy in direct:
            copy.start()
        vec_f[pl.ds(place, 1)] = (settled[0:1] + lift(slope[...], coming_c))[None]
        for copy in f_copies:
            copy.start()

    held, forward_gain = middle(held_in + lift(tails[place], coming_c))

    @pl.when(jnp.logical_not(sends_direct))
    def _():
        vec_f[pl.ds(place, 1)] = end_term()[None]
        for copy in f_copies:
            copy.start()

    turned_r[...] = heads[place].T

    @pl.when(jnp.logical_and(first_group, me > 0))
    def _():
        for k in range(sections):
            fb_t[k] = turned(fb[k])


    drive = jnp.concatenate([jnp.zeros((1, ns), F32), pushes[:last]], axis=0) - defect
    drive_t = turned(drive)
    step = drive[0:1]
    kept = [step]
    acc = jnp.zeros((ns, LANES), F32)
    for k in range(1, sections):
        if k % 2:
            block = jnp.broadcast_to(times(m[k - 1], step), (ns, LANES)) + drive_t[:, k:k + 1]
            acc = jnp.where(lane == k, block, acc)
            kept.append(jnp.zeros((1, ns), F32))
        else:
            step = lift(m[k - 1], block) + drive[k:k + 1]
            kept.append(step)
    kept.append(jnp.zeros((LANES - sections, ns), F32))
    cols[...] = acc + jnp.concatenate(kept, axis=0).T

    moved = cols[:, :sections] - defect_t
    acc = jnp.zeros((nu, LANES), F32)
    alone = cols[...].T
    for k in range(sections):
        packed_out[sections + k:sections + k + 1] = times_t(v[k], moved[:, k:k + 1]) + back[k:k + 1]
        acc = jnp.where(lane_u == k, times(fb[k], alone[k:k + 1]), acc)
    fed_local[...] = turned(acc)[:sections]

    starts = me == 0

    @pl.when(jnp.logical_not(starts))
    def _():
        arrive(vec_f, f_send, f_recv)
        held_on = jnp.zeros((1, ns), F32)
        y = vec_f[0]
        for e in range(1, size):
            held_on = jnp.where(place == e, y, held_on)
            y = vec_f[e] + row_of(times(group[e], y))
        joins[...] = packed(y, held_on)

    @pl.when(starts)
    def _():
        joins[...] = jnp.zeros_like(joins)

    @pl.when(first_group)
    def _():
        ch_f_in[...] = jnp.zeros_like(ch_f_in)

    @pl.when(at_group == 1)
    def _():
        came = jnp.zeros((1, ns), F32)
        for j in range(size):
            remote(direct_out, direct_in.at[j], d_send.at[j], d_recv.at[j],
                   base - size + j).wait_recv()
            came = came + direct_in[j, 0:1]
        ch_f_in[...] = packed(came, direct_in[0, 1:2])

    @pl.when(to_top)
    def _():
        own_g[...] = packed(joins[0:1], group_stats)
        up_g.start()

    @pl.when(jnp.logical_and(at_group > 1, jnp.logical_not(skipped)))
    def _():
        to_after.wait_recv()

    @pl.when(skipped)
    def _():
        up_w.wait_recv()
        up_g.wait_recv()
        up_skip.wait_recv()
        ch_f_in[...] = packed(
            skip_g[0:1] + lift(skip_w[...], column_block(skip_in[0:1])), skip_g[1:2] + skip_in[1:2]
        )

    below = ch_f_in[1:2]
    entering_c = column_block(ch_f_in[0:1])
    goes_on = jnp.logical_not(jnp.logical_or(jnp.logical_or(first_group, top_group), to_top))

    @pl.when(goes_on)
    def _():
        ch_f_out[...] = packed(joins[0:1] + lift(turned_w[...], entering_c), below + group_stats)
        to_after.start()

    @pl.when(to_skip)
    def _():
        up_skip.start()

    entering = joins[1:2] + lift(turned_r[...], entering_c)

    @pl.when(starts)
    def _():
        packed_out[0:sections] = cols[...].T[:sections]

    @pl.when(jnp.logical_not(starts))
    def _():
        acc = jnp.zeros((ns, LANES), F32)
        fed = []
        for k in range(sections):
            if k:
                block = jnp.broadcast_to(times(pre[k - 1], entering), (ns, LANES))
            else:
                block = column_block(entering)
            acc = jnp.where(lane == k, block, acc)
            packed_out[sections + k:sections + k + 1] = (
                packed_out[sections + k:sections + k + 1] + lift(v[k], block)
            )
            fed.append(lift(fb_t[k], block))
        packed_out[0:sections] = (cols[...] + acc).T[:sections]
        fed_local[...] = fed_local[...] + jnp.concatenate(fed, axis=0)

    fed = fed_local[...]
    chosen = ac[...].astype(F32)
    input_step = (1.0 - chosen) * (fed + forward_gain) + chosen * (ub[...] - inp[...])
    bound_step = chosen * (
        held + jnp.dot(input_step, w[...], precision=PRECISE, preferred_element_type=F32)
    )
    packed_out[2 * sections:3 * sections] = jnp.concatenate(
        [input_step, bound_step, jnp.zeros((sections, ns - 2 * nu), F32)], axis=1
    )
    totals = above + group_stats + below
    tops = totals[:, 0:3]
    scale = totals[:, 3:6]
    spot = lax.broadcasted_iota(jnp.int32, (1, 3), 1)
    horizon = sections * n
    entries = jnp.where(spot == 0, ns, jnp.where(spot == 1, ns + nu, nu)).astype(F32)
    norms = jnp.sqrt(tops / (scale + floor_share * horizon * entries))
    packed_out[3 * sections:3 * sections + 1, 0:3] = norms

    @pl.when(starts)
    def _():
        arrive(vec_f, f_send, f_recv)

    @pl.when(me > 0)
    def _():
        to_earlier.wait_send()

    @pl.when(me < n - 1)
    def _():
        to_later.wait_send()

    for copy in p_copies + b_copies + f_copies:
        copy.wait_send()

    @pl.when(jnp.logical_or(jnp.logical_and(top_group, jnp.logical_not(first_group)), carries))
    def _():
        to_before.wait_send()

    if paired:
        @pl.when(jnp.logical_and(served, top_group))
        def _():
            enter_twin.wait_send()

        @pl.when(gives)
        def _():
            give_w.wait_send()

        @pl.when(helps)
        def _():
            hand_back.wait_send()

        @pl.when(hops_on)
        def _():
            pass_on.wait_send()

    @pl.when(sends_direct)
    def _():
        for copy in direct:
            copy.wait_send()

    @pl.when(goes_on)
    def _():
        to_after.wait_send()

    @pl.when(to_skip)
    def _():
        up_skip.wait_send()

    @pl.when(to_top)
    def _():
        up_w.wait_send()
        up_g.wait_send()


def spread(sections, ns, nu, packed, o_state, o_input, o_mult, o_bound, o_norm):
    o_state[...] = packed[0:sections]
    o_mult[...] = packed[sections:2 * sections]
    o_input[...] = packed[2 * sections:3 * sections, 0:nu]
    o_bound[...] = packed[2 * sections:3 * sections, nu:2 * nu]
    o_norm[...] = packed[3 * sections:3 * sections + 1, 0:3]


def local(n, parts, *args):
    size = 4 if n % 4 == 0 else (2 if n % 2 == 0 else 1)
    sections, ns = args[12].shape
    nu = args[13].shape[1]
    mates = size - 1
    copies = [pltpu.VMEM(x.shape, x.dtype) for x in args]
    dma = pltpu.SemaphoreType.DMA
    scratch = copies + [
        pltpu.VMEM((sections, ns, ns), F32),
        pltpu.VMEM((sections, ns, ns), F32),
        pltpu.VMEM((size, ns, ns), F32),
        pltpu.VMEM((size + 1, ns, ns), F32),
        pltpu.VMEM((size, ns, ns), F32),
        pltpu.VMEM((ns, ns), F32),
        pltpu.VMEM((ns, ns), F32),
        pltpu.VMEM((ns, ns), F32),
        pltpu.VMEM((ns, ns), F32),
        pltpu.VMEM((sections * nu, ns), F32),
        pltpu.VMEM((sections * nu, ns), F32),
        pltpu.VMEM((sections, ns, nu), F32),
        pltpu.VMEM((sections, nu), F32),
        pltpu.VMEM((2, ns), F32),
        pltpu.VMEM((sections, ns), F32),
        pltpu.VMEM((sections, ns), F32),
        pltpu.VMEM((sections, ns), F32),
        pltpu.VMEM((sections, ns), F32),
        pltpu.VMEM((ns, LANES), F32),
    ] + [pltpu.VMEM((1, ns), F32)] * 4 + [
        pltpu.VMEM((size, 2, ns), F32),
        pltpu.VMEM((size, 1, ns), F32),
        pltpu.VMEM((size, 2, ns), F32),
    ] + [pltpu.VMEM((2, ns), F32)] * 6 + [
        pltpu.VMEM((ns, ns), F32), pltpu.VMEM((2, ns), F32), pltpu.VMEM((2, ns), F32),
    ] + [pltpu.VMEM((2, ns), F32)] * 3 + [
        pltpu.VMEM((ns, ns), F32), pltpu.VMEM((2, ns), F32),
        dma((18,)), dma((sections,)), dma((2,)), dma((2,)),
        dma((6,)), dma((6,)), dma((mates,)), dma((mates,)), dma((mates,)), dma((mates,)),
        dma((size,)), dma((size,)), dma((2,)), dma((2,)), dma((3,)), dma((3,)), dma((4,)), dma((3,)),
    ]
    args = [pltpu.with_memory_space_constraint(x, pltpu.HBM) for x in args]
    packed = pl.pallas_call(
        functools.partial(kernel, n, size, parts),
        out_shape=jax.ShapeDtypeStruct((3 * sections + 8, ns), F32),
        in_specs=[pl.BlockSpec(memory_space=pltpu.HBM)] * len(args),
        out_specs=pl.BlockSpec(memory_space=pltpu.VMEM),
        scratch_shapes=scratch,
        compiler_params=pltpu.CompilerParams(
            collective_id=0, has_side_effects=True, vmem_limit_bytes=VMEM_LIMIT
        ),
    )(*args)
    outs = [(sections, ns), (sections, nu), (sections, ns), (sections, nu), (1, 3)]
    results = pl.pallas_call(
        functools.partial(spread, sections, ns, nu),
        out_shape=[jax.ShapeDtypeStruct(shape, F32) for shape in outs],
        in_specs=[pl.BlockSpec(memory_space=pltpu.VMEM)],
        out_specs=[pl.BlockSpec(memory_space=pltpu.VMEM)] * len(outs),
        compiler_params=pltpu.CompilerParams(vmem_limit_bytes=4 * 1024 * 1024),
    )(packed)
    return (*results[:4], results[4][0])


def solution(mesh):
    wide = P(("batch", "tm"), None, None)
    flat = P(("batch", "tm"), None)
    in_specs = (wide,) * 6 + (P("batch", None),) + (flat,) * 10
    out_specs = (flat,) * 4 + (P("batch"),)
    return jax.shard_map(
        functools.partial(local, mesh.shape["tm"], mesh.shape["batch"]),
        mesh=mesh, in_specs=in_specs, out_specs=out_specs, check_vma=False,
    )
```
